256 devices in a mesh: lat: 16 (over z, y_lo), lev: 16 (over y_hi, x, core).
Axes of the slice: x: 4, y: 4 (y_hi: 2, y_lo: 2; y = y_hi * 2 + y_lo), z: 8, core: 2. Of those that a mesh axis runs over, the one named last changes fastest.
Arguments:
- tracer: float32 [2, 16, 768, 1152], P(None, 'lev', 'lat'), may hold values from 0.1 to 2
- east_courant: float32 [16, 768, 1152], P('lev', 'lat'), may hold values from -0.8 to 0.8
- north_courant: float32 [16, 768, 1152], P('lev', 'lat'), may hold values from -0.8 to 0.8
- fall_speed: float32 [2, 16, 768, 1152], P(None, 'lev', 'lat'), may hold values from 0.05 to 0.6
Outputs:
- tracer_out: float32 [2, 16, 768, 1152], P(None, 'lev', 'lat')
- deposit: float32 [2, 768, 1152], P(None, 'lat', 'lev')
The draws below stay inside these ranges and needn't reach their ends.
All inputs are finite; a program needn't handle non-finite values.
Results may differ from the reference program's by a relative error of at most 0.0003.
Values sent between devices are 32-bit elements; how exact they have to be, the bound alone decides.
A program may use at most 64 MiB of HBM per device.

```python
import math
import jax
import jax.numpy as jnp
from jax import lax

BINS = 2
NLON = 1152
HSUB = 4
SETTLE_SUBSTEPS = 6
LEV = 16
NLAT = 768


def levels(rng, extent, pieces, smallest, largest):
    loudness, own = 1.0, jax.random.fold_in(rng, 6)
    for position, blocks in pieces:
        heights = jnp.exp(jax.random.uniform(jax.random.fold_in(own, position), (blocks,), jnp.float32, smallest / len(pieces), largest / len(pieces)))
        loudness = loudness * jnp.repeat(heights, extent[position] // blocks).reshape([-1 if axis == position else 1 for axis in range(len(extent))])
    return loudness


def setup_inputs(seed: int = 0) -> dict:
    key_of = jax.random.split(jax.random.key(seed), 5)
    return {
        "tracer": jnp.clip(0.1 + 1.9 * jax.random.uniform(key_of[0], (BINS, LEV, NLAT, NLON), jnp.float32) ** levels(key_of[0], (BINS, LEV, NLAT, NLON), ((1, 16), (2, 16)), -0.2, 0.2), 0.1, 2.0),
        "east_courant": jnp.clip(jax.random.uniform(key_of[1], (LEV, NLAT, NLON), jnp.float32, -0.8, 0.8) * levels(key_of[1], (LEV, NLAT, NLON), ((0, 16), (1, 16)), -0.4, 0.0), -0.8, 0.8),
        "north_courant": jnp.clip(jax.random.uniform(key_of[2], (LEV, NLAT, NLON), jnp.float32, -0.8, 0.8) * levels(key_of[2], (LEV, NLAT, NLON), ((0, 16), (1, 16)), -0.4, 0.0), -0.8, 0.8),
        "fall_speed": jnp.clip(jnp.exp(math.log(0.6) - 2.4849067 * jax.random.uniform(key_of[3], (BINS, LEV, NLAT, NLON), jnp.float32) ** levels(key_of[3], (BINS, LEV, NLAT, NLON), ((1, 16), (2, 16)), -0.2, 0.2)), 0.05, 0.6),
    }


def limiter_face_value(outer_west, inner_west, inner_east, outer_east):
    interp = (7.0 / 12.0) * (inner_west + inner_east) - (1.0 / 12.0) * (outer_west + outer_east)
    return jnp.clip(interp, jnp.minimum(inner_west, inner_east), jnp.maximum(inner_west, inner_east))


def window_for_cell(source, start, length, axis_dim):
    return lax.slice_in_dim(source, start, start + length, axis=axis_dim)


def sweep(halo_padded_field, courant, axis_dim):
    cells = halo_padded_field.shape[axis_dim] - 6
    faces = limiter_face_value(window_for_cell(halo_padded_field, 0, cells + 3, axis_dim), window_for_cell(halo_padded_field, 1, cells + 3, axis_dim),
                         window_for_cell(halo_padded_field, 2, cells + 3, axis_dim), window_for_cell(halo_padded_field, 3, cells + 3, axis_dim))
    middle = window_for_cell(halo_padded_field, 2, cells + 2, axis_dim)
    west_face = window_for_cell(faces, 0, cells + 2, axis_dim)
    east_face = window_for_cell(faces, 1, cells + 2, axis_dim)
    spread = east_face - west_face
    curvature = 6.0 * middle - 3.0 * (west_face + east_face)
    courant_abs = jnp.abs(courant)
    shape_term = 1.0 - (2.0 / 3.0) * courant_abs
    from_west = window_for_cell(east_face, 0, cells + 1, axis_dim) - 0.5 * courant_abs * (
        window_for_cell(spread, 0, cells + 1, axis_dim) - shape_term * window_for_cell(curvature, 0, cells + 1, axis_dim))
    from_east = window_for_cell(west_face, 1, cells + 1, axis_dim) + 0.5 * courant_abs * (
        window_for_cell(spread, 1, cells + 1, axis_dim) + shape_term * window_for_cell(curvature, 1, cells + 1, axis_dim))
    face_flux_values = courant * jnp.where(courant >= 0, from_west, from_east)
    return window_for_cell(halo_padded_field, 3, cells, axis_dim) - (window_for_cell(face_flux_values, 1, cells, axis_dim) - window_for_cell(face_flux_values, 0, cells, axis_dim))


def zonal(field, east_courant):
    last_dim = field.ndim - 1
    width = field.shape[last_dim]
    halo_padded_field = jnp.concatenate([window_for_cell(field, width - 3, 3, last_dim), field, window_for_cell(field, 0, 3, last_dim)], last_dim)
    cour_dim = east_courant.ndim - 1
    courant = jnp.concatenate([window_for_cell(east_courant, width - 1, 1, cour_dim), east_courant], cour_dim)
    return sweep(halo_padded_field, courant, last_dim)


def horizontal(field, east_courant, face_cour):
    field = zonal(field, east_courant)
    halo_padded_field = jnp.pad(field, ((0, 0), (3, 3), (0, 0)))
    return sweep(halo_padded_field, face_cour, 1)


def settle(column_mass, fall_speed):
    deposit = jnp.zeros_like(column_mass[:, 0])
    for settle_substep in range(SETTLE_SUBSTEPS):
        speeds = fall_speed * (1.0 + 0.5 * jnp.tanh(column_mass))
        face_flux_values = speeds * column_mass
        inflow = jnp.concatenate([jnp.zeros_like(face_flux_values[:, :1]), face_flux_values[:, :-1]], 1)
        column_mass = (column_mass + inflow) - face_flux_values
        deposit = deposit + face_flux_values[:, -1]
    return column_mass, deposit


def reference(tracer, east_courant, north_courant, fall_speed):
    row_ids = jnp.arange(NLAT, dtype=jnp.int32)
    north_faces = jnp.where((row_ids == NLAT - 1)[None, :, None], jnp.zeros_like(north_courant), north_courant)
    face_cour = jnp.concatenate([jnp.zeros_like(north_faces[:, :1]), north_faces], 1)

    def advect_many(inputs):
        field, east_level, face_level = inputs
        for settle_substep in range(HSUB):
            field = horizontal(field, east_level, face_level)
        return field

    def advect_once(inputs):
        field, east_level, face_level = inputs
        return horizontal(field, east_level, face_level)

    by_level = lax.map(advect_many, (jnp.moveaxis(tracer, 1, 0), east_courant, face_cour))
    settled, deposit = settle(jnp.moveaxis(by_level, 0, 1), fall_speed)
    closing = lax.map(advect_once, (jnp.moveaxis(settled, 1, 0), east_courant, face_cour))
    return jnp.moveaxis(closing, 0, 1), deposit
```

```python
import functools

import jax
import jax.numpy as jnp
from jax import lax
from jax.experimental import pallas as pl
from jax.experimental.pallas import tpu as pltpu
from jax.sharding import PartitionSpec as P

HSUB = 4
SETTLE_SUBSTEPS = 6
SUB = 8
LANE = 128
MESH = pl.DeviceIdType.MESH
VMEM = pltpu.VMEM
DMA = pltpu.SemaphoreType.DMA


def coefficients(k):
    s = jnp.abs(k)
    half = 0.5 * k * s
    a3 = 3.0 * half * (1.0 - (2.0 / 3.0) * s)
    return k - a3 - half, 2.0 * a3, half - a3


def face_value(a, b, c, d):
    value = (7.0 / 12.0) * (b + c) - (1.0 / 12.0) * (a + d)
    return jnp.minimum(jnp.maximum(value, jnp.minimum(b, c)), jnp.maximum(b, c))


def row_of(ref, index, tiles):
    return jnp.concatenate([ref[index + v] for v in range(tiles)], axis=1)


def kernel(
    bands, levels,
    tracer, east, north, fall, out, deposit,
    flat, q, z, q2, cz, cm, hs, hr, ns, nr, fs, rf, rw, so, dp, dr,
    in_sem, out_sem, hs_sem, hr_sem, n_sem, fs_sem, fr_sem, ws_sem, wr_sem, bs_sem, br_sem, ds_sem, dr_sem,
):
    bins, rows, width = tracer.shape
    tall = rows // SUB
    wide = width // LANE
    groups = bins * tall
    tiles = groups * wide
    share = so.shape[1]
    chunk = deposit.shape[2]
    band = lax.axis_index("lat")
    me = lax.axis_index("lev")
    has_south, has_north = band > 0, band < bands - 1
    sub = lax.broadcasted_iota(jnp.int32, (SUB, LANE), 0)
    first, last = sub == 0, sub == SUB - 1

    def peer(k):
        return lax.rem(me + k, levels)

    barrier = pltpu.get_barrier_semaphore()
    for k in range(1, levels):
        pl.semaphore_signal(barrier, inc=1, device_id={"lev": peer(k)}, device_id_type=MESH)

    @pl.when(has_south)
    def _():
        pl.semaphore_signal(barrier, inc=1, device_id={"lat": band - 1}, device_id_type=MESH)

    @pl.when(has_north)
    def _():
        pl.semaphore_signal(barrier, inc=1, device_id={"lat": band + 1}, device_id_type=MESH)

    def fetch(source, slot):
        return [
            pltpu.make_async_copy(
                source.at[:, pl.ds(v * LANE, LANE)], flat.at[slot, v], in_sem.at[slot, v]
            )
            for v in range(wide)
        ]

    fetched = [fetch(north, 0), fetch(east, 1)]
    fetched += [fetch(tracer.at[b], 2 + b) for b in range(bins)]
    fetched += [fetch(fall.at[b], 2 + bins + b) for b in range(bins)]
    for copies in fetched:
        for copy in copies:
            copy.start()
    for copies in fetched:
        for copy in copies:
            copy.wait()

    for j in range(tall):
        for v in range(wide):
            picked = pl.ds(j, SUB, stride=tall)
            k = flat[0, v, picked, :]
            if j == tall - 1:
                k = jnp.where(jnp.logical_and(last, band == bands - 1), 0.0, k)
                ns[v : v + 1, :] = k[SUB - 1 :, :]
            cm[3, j + 1, v] = k
            for i, c in enumerate(coefficients(flat[1, v, picked, :])):
                cz[i, j, v] = c
            for b in range(bins):
                index = (b * tall + j) * wide + v
                q[index] = flat[2 + b, v, picked, :]
                fs[index] = flat[2 + bins + b, v, picked, :]
    for index in range(tiles, q.shape[0]):
        q[index] = jnp.zeros((SUB, LANE), jnp.float32)
        fs[index] = jnp.zeros((SUB, LANE), jnp.float32)

    @pl.when(band == 0)
    def _():
        nr[...] = jnp.zeros_like(nr)
        for s in range(HSUB + 1):
            for b in range(bins):
                hr[s, 0, b] = jnp.zeros(hr.shape[3:], jnp.float32)

    @pl.when(band == bands - 1)
    def _():
        for s in range(HSUB + 1):
            for b in range(bins):
                hr[s, 1, b] = jnp.zeros(hr.shape[3:], jnp.float32)

    pl.semaphore_wait(barrier, levels - 1 + has_south.astype(jnp.int32) + has_north.astype(jnp.int32))

    north_row = pltpu.make_async_remote_copy(
        ns, nr, n_sem.at[0], n_sem.at[1], device_id={"lat": band + 1}, device_id_type=MESH
    )

    @pl.when(has_north)
    def _():
        north_row.start()

    def halo(s, side, b):
        target = band + 1 if side == 0 else band - 1
        return pltpu.make_async_remote_copy(
            hs.at[s, side, b], hr.at[s, side, b], hs_sem.at[s, side, b], hr_sem.at[s, side, b],
            device_id={"lat": target}, device_id_type=MESH,
        )

    def deal(source, target, send_sem, recv_sem, k):
        return pltpu.make_async_remote_copy(
            source.at[pl.ds(peer(k) * share, share)], target.at[me], send_sem.at[k], recv_sem.at[me],
            device_id={"lev": peer(k)}, device_id_type=MESH,
        )

    def dealt(source, target, send_sem, recv_sem, k):
        return pltpu.make_async_remote_copy(
            source.at[pl.ds(me * share, share)], target.at[peer(k)], send_sem.at[k], recv_sem.at[peer(k)],
            device_id={"lev": peer(k)}, device_id_type=MESH,
        )

    def zonal(s, b, field):
        for j in range(tall):
            base = (b * tall + j) * wide
            mid = row_of(field, base, wide)
            west = pltpu.roll(mid, 1, 1)
            east_1 = pltpu.roll(mid, width - 1, 1)
            east_2 = pltpu.roll(mid, width - 2, 1)
            face = face_value(west, mid, east_1, east_2)
            c0 = jnp.concatenate([cz[0, j, v] for v in range(wide)], axis=1)
            c1 = jnp.concatenate([cz[1, j, v] for v in range(wide)], axis=1)
            c2 = jnp.concatenate([cz[2, j, v] for v in range(wide)], axis=1)
            up = c1 >= 0
            flux = (
                c0 * face
                + c1 * jnp.where(up, mid, east_1)
                + c2 * jnp.where(up, pltpu.roll(face, 1, 1), pltpu.roll(face, width - 1, 1))
            )
            new = mid - (flux - pltpu.roll(flux, 1, 1))
            for v in range(wide):
                z[base + v] = new[:, v * LANE : (v + 1) * LANE]
                if j < 3:
                    hs[s, 1, b, pl.ds(j * wide + v, 1), :] = new[:1, v * LANE : (v + 1) * LANE]
                if j >= tall - 3:
                    hs[s, 0, b, pl.ds((j - tall + 3) * wide + v, 1), :] = new[SUB - 1 :, v * LANE : (v + 1) * LANE]

        @pl.when(has_north)
        def _():
            halo(s, 0, b).start()

        @pl.when(has_south)
        def _():
            halo(s, 1, b).start()

    def meridional(s, b, store):
        @pl.when(has_south)
        def _():
            halo(s, 0, b).wait_recv()

        @pl.when(has_north)
        def _():
            halo(s, 1, b).wait_recv()

        for v in range(wide):
            own = [z[(b * tall + j) * wide + v] for j in range(tall)]
            below = [
                jnp.where(first, hr[s, 0, b, pl.ds(i * wide + v, 1), :], pltpu.roll(own[tall - 3 + i], 1, 0))
                for i in range(3)
            ]
            above = [
                jnp.where(last, hr[s, 1, b, pl.ds(i * wide + v, 1), :], pltpu.roll(own[i], SUB - 1, 0))
                for i in range(3)
            ]
            ext = jnp.stack(below + own + above)
            face = face_value(ext[: tall + 3], ext[1 : tall + 4], ext[2 : tall + 5], ext[3:])
            c0, c1, c2 = cm[0, :, v], cm[1, :, v], cm[2, :, v]
            up = c1 >= 0
            flux = (
                c0 * face[1 : tall + 2]
                + c1 * jnp.where(up, ext[2 : tall + 3], ext[3 : tall + 4])
                + c2 * jnp.where(up, face[: tall + 1], face[2:])
            )
            new = ext[3 : tall + 3] - (flux[1:] - flux[:-1])
            for j in range(tall):
                store(b, j, v, new[j])

    def keep(b, j, v, tile):
        q[(b * tall + j) * wide + v] = tile

    def finish(b, j, v, tile):
        flat[b, v, pl.ds(j, SUB, stride=tall), :] = tile

    per_step = -(-levels // HSUB)

    def substep(s, carry):
        for b in range(bins):
            zonal(s, b, q)
        for i in range(per_step):
            k = s * per_step + i

            @pl.when(jnp.logical_and(k > 0, k < levels))
            def _():
                deal(fs, rf, fs_sem, fr_sem, k).start()

        @pl.when(s == 0)
        def _():
            @pl.when(has_south)
            def _():
                north_row.wait_recv()

            for v in range(wide):
                low = jnp.where(first, nr[v : v + 1, :], pltpu.roll(cm[3, tall, v], 1, 0))
                for j in range(tall + 1):
                    for i, c in enumerate(coefficients(cm[3, j, v] if j else low)):
                        cm[i, j, v] = c

        for b in range(bins):
            meridional(s, b, keep)
        return carry

    lax.fori_loop(0, HSUB, substep, 0)

    for k in range(1, levels):
        deal(q, rw, ws_sem, wr_sem, k).start()
    for i in range(share):
        rw[me, i] = q[me * share + i]
        rf[me, i] = fs[me * share + i]
    for k in range(1, levels):
        dealt(fs, rf, fs_sem, fr_sem, k).wait_recv()
    for k in range(1, levels):
        dealt(q, rw, ws_sem, wr_sem, k).wait_recv()

    def settle(i, carry):
        mass = rw[:, i]
        half = 0.5 * rf[:, i]
        fallen = jnp.zeros((SUB, LANE), jnp.float32)
        for _ in range(SETTLE_SUBSTEPS):
            flux = (mass * half) * (2.0 + jnp.tanh(mass))
            inflow = jnp.concatenate([jnp.zeros((1, SUB, LANE), jnp.float32), flux[:-1]], axis=0)
            mass = (mass + inflow) - flux
            fallen = fallen + flux[levels - 1]
        so[:, i] = mass
        dp[i] = fallen
        return carry

    lax.fori_loop(0, share, settle, 0)

    def give_back(k):
        return pltpu.make_async_remote_copy(
            so.at[peer(k)], q2.at[pl.ds(me * share, share)], bs_sem.at[k], br_sem.at[me],
            device_id={"lev": peer(k)}, device_id_type=MESH,
        )

    def given_back(k):
        return pltpu.make_async_remote_copy(
            so.at[peer(k)], q2.at[pl.ds(peer(k) * share, share)], bs_sem.at[k], br_sem.at[peer(k)],
            device_id={"lev": peer(k)}, device_id_type=MESH,
        )

    for k in range(1, levels):
        give_back(k).start()
    for i in range(share):
        q2[me * share + i] = so[me, i]

    reach = max((LANE * v + LANE - 1) // chunk - (LANE * v) // chunk for v in range(wide)) + 1

    def sent(i, e):
        tile = me * share + i
        v = lax.rem(tile, wide)
        target = (LANE * v) // chunk + e
        valid = jnp.logical_and(tile < tiles, target <= (LANE * v + LANE - 1) // chunk)
        slot = (tile // wide) * 2 + v - (chunk * target) // LANE
        return target, valid, slot

    def drop(i, e):
        target, valid, slot = sent(i, e)
        away = jnp.logical_and(valid, target != me)
        copy = pltpu.make_async_remote_copy(
            dp.at[i], dr.at[slot], ds_sem.at[i, e], dr_sem.at[slot],
            device_id={"lev": target}, device_id_type=MESH,
        )
        return copy, away

    for i in range(share):
        for e in range(reach):
            copy, away = drop(i, e)
            target, valid, slot = sent(i, e)

            @pl.when(away)
            def _():
                copy.start()

            @pl.when(jnp.logical_and(valid, target == me))
            def _():
                dr[slot] = dp[i]

    for k in range(1, levels):
        given_back(k).wait_recv()

    for b in range(bins):
        zonal(HSUB, b, q2)
    written = [
        [
            pltpu.make_async_copy(
                flat.at[b, v], out.at[b, :, pl.ds(v * LANE, LANE)], out_sem.at[b, v]
            )
            for v in range(wide)
        ]
        for b in range(bins)
    ]
    for b in range(bins):
        meridional(HSUB, b, finish)
        for copy in written[b]:
            copy.start()

    low_tile = (chunk * me) // LANE
    high_tile = (chunk * me + chunk - 1) // LANE
    offset = chunk * me - LANE * low_tile
    for g in range(groups):
        for e in range(2):
            slot = 2 * g + e
            tile = g * wide + low_tile + e
            used = low_tile + e <= high_tile
            source = tile // share

            @pl.when(jnp.logical_and(used, source != me))
            def _():
                pltpu.make_async_remote_copy(
                    dp.at[0], dr.at[slot], ds_sem.at[0, 0], dr_sem.at[slot],
                    device_id={"lev": lax.rem(me + 1, levels)}, device_id_type=MESH,
                ).wait_recv()

            @pl.when(jnp.logical_not(used))
            def _():
                dr[slot] = jnp.zeros((SUB, LANE), jnp.float32)

        both = jnp.concatenate([dr[2 * g], dr[2 * g + 1]], axis=1)
        both = pltpu.roll(both, lax.rem(2 * LANE - offset, 2 * LANE), 1)
        flat[bins + g // tall, 0, pl.ds(g % tall, SUB, stride=tall), :] = both[:, :LANE]
    for b in range(bins):
        deposit[b] = flat[bins + b, 0][:, :chunk]
    for copies in written:
        for copy in copies:
            copy.wait()

    @pl.when(has_north)
    def _():
        north_row.wait_send()

    for s in range(HSUB + 1):
        for b in range(bins):
            @pl.when(has_north)
            def _():
                halo(s, 0, b).wait_send()

            @pl.when(has_south)
            def _():
                halo(s, 1, b).wait_send()

    for k in range(1, levels):
        deal(fs, rf, fs_sem, fr_sem, k).wait_send()
        deal(q, rw, ws_sem, wr_sem, k).wait_send()
        give_back(k).wait_send()
    for i in range(share):
        for e in range(reach):
            copy, away = drop(i, e)

            @pl.when(away)
            def _():
                copy.wait_send()


def on_device(bands, levels, tracer, east, north, fall):
    bins, _, rows, width = tracer.shape
    tall, wide = rows // SUB, width // LANE
    tiles = bins * tall * wide
    share = -(-tiles // levels)
    chunk = width // levels
    reach = max((LANE * v + LANE - 1) // chunk - (LANE * v) // chunk for v in range(wide)) + 1
    edge = -(-3 * wide // SUB) * SUB
    line = -(-wide // SUB) * SUB
    steps = HSUB + 1
    f32 = jnp.float32
    out, deposit = pl.pallas_call(
        functools.partial(kernel, bands, levels),
        out_shape=(
            jax.ShapeDtypeStruct((bins, rows, width), f32),
            jax.ShapeDtypeStruct((bins, rows, chunk), f32),
        ),
        in_specs=[pl.BlockSpec(memory_space=pltpu.HBM)] * 4,
        out_specs=(pl.BlockSpec(memory_space=pltpu.HBM), pl.BlockSpec(memory_space=VMEM)),
        scratch_shapes=[
            VMEM((2 + 2 * bins, wide, rows, LANE), f32),
            VMEM((share * levels, SUB, LANE), f32),
            VMEM((tiles, SUB, LANE), f32),
            VMEM((share * levels, SUB, LANE), f32),
            VMEM((3, tall, wide, SUB, LANE), f32),
            VMEM((4, tall + 1, wide, SUB, LANE), f32),
            VMEM((steps, 2, bins, edge, LANE), f32),
            VMEM((steps, 2, bins, edge, LANE), f32),
            VMEM((line, LANE), f32),
            VMEM((line, LANE), f32),
            VMEM((share * levels, SUB, LANE), f32),
            VMEM((levels, share, SUB, LANE), f32),
            VMEM((levels, share, SUB, LANE), f32),
            VMEM((levels, share, SUB, LANE), f32),
            VMEM((share, SUB, LANE), f32),
            VMEM((2 * bins * tall, SUB, LANE), f32),
            DMA((2 + 2 * bins, wide)),
            DMA((bins, wide)),
            DMA((steps, 2, bins)),
            DMA((steps, 2, bins)),
            DMA((2,)),
            DMA((levels,)),
            DMA((levels,)),
            DMA((levels,)),
            DMA((levels,)),
            DMA((levels,)),
            DMA((levels,)),
            DMA((share, reach)),
            DMA((2 * bins * tall,)),
        ],
        compiler_params=pltpu.CompilerParams(
            collective_id=0, has_side_effects=True, vmem_limit_bytes=32 * 1024 * 1024
        ),
        cost_estimate=pl.CostEstimate(flops=50000000, bytes_accessed=3000000, transcendentals=700000),
    )(
        tracer.reshape(bins, rows, width),
        east.reshape(rows, width),
        north.reshape(rows, width),
        fall.reshape(bins, rows, width),
    )
    return out.reshape(tracer.shape), deposit


def solution(mesh):
    in_specs = (
        P(None, "lev", "lat", None),
        P("lev", "lat", None),
        P("lev", "lat", None),
        P(None, "lev", "lat", None),
    )
    out_specs = (P(None, "lev", "lat", None), P(None, "lat", "lev"))
    return jax.shard_map(
        functools.partial(on_device, mesh.shape["lat"], mesh.shape["lev"]),
        mesh=mesh, in_specs=in_specs, out_specs=out_specs, check_vma=False,
    )
```

```python
import functools

import jax
import jax.numpy as jnp
from jax import lax
from jax.experimental import pallas as pl
from jax.experimental.pallas import tpu as pltpu
from jax.sharding import PartitionSpec as P

HSUB = 4
SETTLE_SUBSTEPS = 6
SUB = 8
LANE = 128
MESH = pl.DeviceIdType.MESH
VMEM = pltpu.VMEM
DMA = pltpu.SemaphoreType.DMA
scope = jax.named_scope


def coefficients(k):
    s = jnp.abs(k)
    half = 0.5 * k * s
    a3 = 3.0 * half * (1.0 - (2.0 / 3.0) * s)
    return k - a3 - half, 2.0 * a3, half - a3


def swept(ext, c0, c1, c2):
    n = ext.shape[0] - 6
    b, c = ext[1 : n + 4], ext[2 : n + 5]
    face = (7.0 / 12.0) * (b + c) - (1.0 / 12.0) * (ext[: n + 3] + ext[3:])
    face = jnp.minimum(jnp.maximum(face, jnp.minimum(b, c)), jnp.maximum(b, c))
    up = c1 >= 0
    flux = (
        c0 * face[1 : n + 2]
        + c1 * jnp.where(up, ext[2 : n + 3], ext[3 : n + 4])
        + c2 * jnp.where(up, face[: n + 1], face[2:])
    )
    return ext[3 : n + 3] - (flux[1:] - flux[:-1])


def kernel(
    bands, levels,
    tracer, east, north, fall, out, deposit,
    flat, turn, q, z, q2, q3, fs, cz, cm, hs, hr, ns, nr, rf, rw, so, dblk, dts, dr,
    in_sem, out_sem, hs_sem, hr_sem, n_sem, f_sem, w_sem, b_sem, d_sem,
):
    bins, rows, width = tracer.shape
    tall = rows // SUB
    wide = width // LANE
    main = tall * (wide - 1) // levels
    each = main + 1
    spare = 1 if bins * tall <= levels else bins
    share = main * bins + spare
    across = levels // 4
    lanes_each = LANE // levels
    chunk = width // levels
    groups = [(b, j) for b in range(bins) for j in range(tall)]
    band = lax.axis_index("lat")
    me = lax.axis_index("lev")
    has_south, has_north = band > 0, band < bands - 1
    sub = lax.broadcasted_iota(jnp.int32, (SUB, LANE), 0)
    first, last = sub == 0, sub == SUB - 1

    half_at, x_at, core_at = me // (2 * across), lax.rem(me // 2, across), lax.rem(me, 2)
    moves = [
        (h, x, c)
        for h in (1, 0)
        for x in sorted(range(across), key=lambda x: -min(x, across - x))
        for c in range(2)
        if (h, x, c) != (0, 0, 0)
    ]
    n_moves = len(moves)
    same_half = [i for i, m in enumerate(moves) if m[0] == 0]
    other_half = [i for i, m in enumerate(moves) if m[0] == 1]

    def at(h, x, c):
        return (lax.rem(half_at + h, 2) * across + lax.rem(x_at + x, across)) * 2 + lax.rem(core_at + c, 2)

    def to(i):
        return at(*moves[i])

    def origin(i):
        h, x, c = moves[i]
        return at(h, across - x, c)

    barrier = pltpu.get_barrier_semaphore()
    for i in range(n_moves):
        pl.semaphore_signal(barrier, inc=1, device_id={"lev": to(i)}, device_id_type=MESH)

    @pl.when(has_south)
    def _():
        pl.semaphore_signal(barrier, inc=1, device_id={"lat": band - 1}, device_id_type=MESH)

    @pl.when(has_north)
    def _():
        pl.semaphore_signal(barrier, inc=1, device_id={"lat": band + 1}, device_id_type=MESH)

    def fetch(source, slot):
        return [
            pltpu.make_async_copy(
                source.at[:, pl.ds(v * LANE, LANE)], flat.at[slot, v], in_sem.at[slot]
            )
            for v in range(wide)
        ]

    fetched = [fetch(tracer.at[b], b) for b in range(bins)] + [fetch(east, bins), fetch(north, bins + 1)]
    fetched += [fetch(fall.at[b], bins + 2 + b) for b in range(bins)]
    for copies in fetched:
        for copy in copies:
            copy.start()

    @pl.when(band == 0)
    def _():
        nr[...] = jnp.zeros_like(nr)
        for s in range(HSUB + 1):
            for b in range(bins):
                hr[0, s, b] = jnp.zeros(hr.shape[3:], jnp.float32)

    @pl.when(band == bands - 1)
    def _():
        for s in range(HSUB + 1):
            for b in range(bins):
                hr[1, s, b] = jnp.zeros(hr.shape[3:], jnp.float32)

    dblk[...] = jnp.zeros_like(dblk)

    def spread(slot, emit):
        for i in range(2):
            pltpu.make_async_copy(flat.at[slot + i], flat.at[slot + i], in_sem.at[slot + i]).wait()
        for v in range(wide):
            block = jnp.concatenate(
                [flat[slot + i, v, pl.ds(j, SUB, stride=tall), :] for i in range(2) for j in range(tall)]
                + [jnp.zeros((LANE - 2 * rows, LANE), jnp.float32)],
                axis=0,
            )
            turn[v * LANE : (v + 1) * LANE, :] = block.T
        for v in range(wide):
            block = turn[pl.ds(v, LANE, stride=wide), :].T
            for i in range(2):
                for j in range(tall):
                    start = (i * tall + j) * SUB
                    emit(i, j, v, block[start : start + SUB])

    def owner(b, j):
        half_tall = tall // 2
        return (tall * b + 2 * (j % half_tall) + (1 if j < half_tall else 0)) % levels

    def extra(b, t):
        u = lax.rem(t + levels * bins - tall * b, levels)
        return u < tall, u // 2 + (tall // 2) * (1 - lax.rem(u, 2))

    def place(b, v, j):
        tile = v * tall + j
        return (tile // main, tile % main) if v < wide - 1 else (owner(b, j), main)

    def index(b, v, j):
        t, i = place(b, v, j)
        return t * each + i

    def emit_tracer(b, j, v, tile):
        q[b, index(b, v, j)] = tile

    def emit_courant(i, j, v, tile):
        if i == 0:
            for n, c in enumerate(coefficients(tile)):
                cz[n, j, v + 1] = c
            return
        if j == tall - 1:
            tile = jnp.where(jnp.logical_and(last, band == bands - 1), 0.0, tile)
            ns[v : v + 1, :] = tile[SUB - 1 :, :]
        for n, c in enumerate(coefficients(tile)):
            cm[n, v, j + 1] = c

    def emit_fall(b, j, v, tile):
        t, i = place(b, v, j)
        fs[t * share + (b * main + i if i < main else bins * main + b % spare)] = tile

    with scope("spread"):
        spread(0, emit_tracer)
        spread(bins, emit_courant)
        for n in range(3):
            for j in range(tall):
                cz[n, j, 0] = pltpu.roll(cz[n, j, wide], 1, 1)

    north_row = pltpu.make_async_remote_copy(
        ns, nr, n_sem.at[0], n_sem.at[1], device_id={"lat": band + 1}, device_id_type=MESH
    )

    def halo(s, side, b):
        target = band + 1 if side == 0 else band - 1
        return pltpu.make_async_remote_copy(
            hs.at[side, s, b], hr.at[side, s, b], hs_sem.at[side], hr_sem.at[s % 2, side, b],
            device_id={"lat": target}, device_id_type=MESH,
        )

    def zonal(s, b, field):
        with scope("zonal"):
            for j in range(tall):
                own = [field[b, index(b, v, j)] for v in range(wide)]
                ext = jnp.stack(
                    [pltpu.roll(t, 1, 1) for t in own[-3:]] + own + [pltpu.roll(t, LANE - 1, 1) for t in own[:3]]
                )
                new = swept(ext, cz[0, j], cz[1, j], cz[2, j])
                for v in range(wide):
                    z[b, v * tall + j] = new[v]
                    if j < 3:
                        hs[1, s, b, pl.ds(j * wide + v, 1), :] = new[v][:1, :]
                    if j >= tall - 3:
                        hs[0, s, b, pl.ds((j - tall + 3) * wide + v, 1), :] = new[v][SUB - 1 :, :]

    def send_halo(s, b):
        @pl.when(has_north)
        def _():
            halo(s, 0, b).start()

        @pl.when(has_south)
        def _():
            halo(s, 1, b).start()

    def meridional(s, b, keep):
        with scope("halo"):
            @pl.when(has_south)
            def _():
                halo(s, 0, b).wait_recv()

            @pl.when(has_north)
            def _():
                halo(s, 1, b).wait_recv()

        with scope("meridional"):
            for v in range(wide):
                own = z[b, v * tall : (v + 1) * tall]
                below = [
                    jnp.where(first, hr[0, s, b, pl.ds(i * wide + v, 1), :], pltpu.roll(own[tall - 3 + i], 1, 0))
                    for i in range(3)
                ]
                above = [
                    jnp.where(last, hr[1, s, b, pl.ds(i * wide + v, 1), :], pltpu.roll(own[i], SUB - 1, 0))
                    for i in range(3)
                ]
                ext = jnp.concatenate([jnp.stack(below), own, jnp.stack(above)])
                new = swept(ext, cm[0, v], cm[1, v], cm[2, v])
                for j in range(tall):
                    keep(b, v, j, new[j])

    def keep_mass(b, v, j, tile):
        q[b, index(b, v, j)] = tile

    def keep_last(b, v, j, tile):
        q3[b, v * tall + j] = tile

    def copy_to(i, source, target, send, recv):
        return pltpu.make_async_remote_copy(
            source, target, send, recv, device_id={"lev": to(i)}, device_id_type=MESH
        )

    def either(condition, yes, no):
        @pl.when(condition)
        def _():
            yes()

        @pl.when(jnp.logical_not(condition))
        def _():
            no()

    def deal_fall(i):
        return copy_to(i, fs.at[pl.ds(to(i) * share, share)], rf.at[me], f_sem.at[0], f_sem.at[1])

    def deal_mass(b, i):
        t = to(i)
        send, recv = w_sem.at[0, b], w_sem.at[1, b]
        either(
            extra(b, t)[0],
            copy_to(i, q.at[b, pl.ds(t * each, each)], rw.at[b, me], send, recv).start,
            copy_to(i, q.at[b, pl.ds(t * each, main)], rw.at[b, me, pl.ds(0, main)], send, recv).start,
        )

    def give_back(b, i):
        t = to(i)
        send, recv = b_sem.at[0, b], b_sem.at[1, b]
        either(
            extra(b, me)[0],
            copy_to(i, so.at[b, t], q2.at[b, pl.ds(me * each, each)], send, recv).start,
            copy_to(i, so.at[b, t, pl.ds(0, main)], q2.at[b, pl.ds(me * each, main)], send, recv).start,
        )

    def settler(b, sems, side):
        full, part = rw.at[b, pl.ds(0, n_moves)], rw.at[b, pl.ds(0, n_moves), pl.ds(0, main)]
        name = "wait_recv" if side else "wait_send"
        either(
            extra(b, me)[0],
            getattr(copy_to(0, full, full, sems.at[0, b], sems.at[1, b]), name),
            getattr(copy_to(0, part, part, sems.at[0, b], sems.at[1, b]), name),
        )

    def holder(b, sems, side):
        count = n_moves * main + tall
        few, many = q.at[b, pl.ds(0, count - 1)], q.at[b, pl.ds(0, count)]
        name = "wait_recv" if side else "wait_send"
        either(
            extra(b, me)[0],
            getattr(copy_to(0, few, few, sems.at[0, b], sems.at[1, b]), name),
            getattr(copy_to(0, many, many, sems.at[0, b], sems.at[1, b]), name),
        )

    all_fall = copy_to(0, rf.at[pl.ds(0, n_moves)], rf.at[pl.ds(0, n_moves)], f_sem.at[0], f_sem.at[1])

    def send_fall(some):
        for i in some:
            deal_fall(i).start()

    per_step = -(-len(other_half) // HSUB)

    for b in range(bins):
        zonal(0, b, q)
    with scope("barrier"):
        pl.semaphore_wait(barrier, n_moves + has_south.astype(jnp.int32) + has_north.astype(jnp.int32))

    @pl.when(has_north)
    def _():
        north_row.start()

    for b in range(bins):
        send_halo(0, b)
    with scope("spread_fall"):
        spread(bins + 2, emit_fall)
    with scope("send_fall"):
        send_fall(same_half + other_half[:per_step])
    for i in range(share):
        rf[me, i] = fs[me * share + i]

    with scope("north_row"):
        @pl.when(has_south)
        def _():
            north_row.wait_recv()

        for v in range(wide):
            below = coefficients(nr[v : v + 1, :])
            for n in range(3):
                cm[n, v, 0] = jnp.where(first, below[n], pltpu.roll(cm[n, v, tall], 1, 0))
    for b in range(bins):
        meridional(0, b, keep_mass)

    for s in range(1, HSUB):
        for b in range(bins):
            zonal(s, b, q)
            send_halo(s, b)
        send_fall(other_half[s * per_step : (s + 1) * per_step])
        for b in range(bins):
            meridional(s, b, keep_mass)
            if s == HSUB - 1:
                for i in range(n_moves):
                    deal_mass(b, i)

    for b in range(bins):
        owned, extra_j = extra(b, me)
        for i in range(main):
            rw[b, me, i] = q[b, me * each + i]

        @pl.when(owned)
        def _():
            rw[b, me, main] = q[b, me * each + main]

        if b == 0:
            with scope("wait_fall"):
                all_fall.wait_recv()
        with scope("wait_mass"):
            settler(b, w_sem, 1)

        def settle(i, j):
            mass = rw[b, :, i]
            half = 0.5 * rf[:, b * main + i if i < main else bins * main + b % spare]
            fallen = jnp.zeros((SUB, LANE), jnp.float32)
            for _ in range(SETTLE_SUBSTEPS):
                flux = (mass * half) * (2.0 + jnp.tanh(mass))
                inflow = jnp.concatenate([jnp.zeros((1, SUB, LANE), jnp.float32), flux[:-1]], axis=0)
                mass = (mass + inflow) - flux
                fallen = fallen + flux[levels - 1]
            so[b, :, i] = mass
            dblk[pl.ds((b * tall + j) * SUB, SUB), :] = fallen

        with scope("settle"):
            for i in range(main):
                settle(i, lax.rem(me * main + i, tall))

            @pl.when(owned)
            def _():
                settle(main, extra_j)

        with scope("give_back"):
            for i in range(n_moves):
                give_back(b, i)
        for i in range(main):
            q2[b, me * each + i] = so[b, me, i]

        @pl.when(owned)
        def _():
            q2[b, me * each + main] = so[b, me, main]

    dts[...] = dblk[...].T

    def drop(i):
        return pltpu.make_async_remote_copy(
            dts.at[pl.ds(to(i) * lanes_each, lanes_each)], dr.at[me], d_sem.at[0], d_sem.at[1],
            device_id={"lev": to(i)}, device_id_type=MESH,
        )

    for i in range(n_moves):
        drop(i).start()
    dr[me] = dts[pl.ds(me * lanes_each, lanes_each), :]

    for b in range(bins):
        with scope("wait_back"):
            holder(b, b_sem, 1)
        zonal(HSUB, b, q2)
        send_halo(HSUB, b)

    with scope("deposit"):
        all_drops = copy_to(0, dr.at[pl.ds(0, n_moves)], dr.at[pl.ds(0, n_moves)], d_sem.at[0], d_sem.at[1])
        all_drops.wait_recv()
        column = lax.broadcasted_iota(jnp.int32, (lanes_each, LANE), 1) // SUB
        low_rows = lax.rem(column, tall) < tall // 2
        for v in range(wide - 1):
            turn[pl.ds(v, lanes_each, stride=wide), :] = jnp.where(low_rows, dr[2 * v], dr[2 * v + 1])
        tail = jnp.zeros((lanes_each, LANE), jnp.float32)
        for g, (b, j) in enumerate(groups):
            t = (tall * b + 2 * (j % (tall // 2)) + (1 if j < tall // 2 else 0)) % levels
            tail = jnp.where(column == g, dr[t], tail)
        turn[pl.ds(wide - 1, lanes_each, stride=wide), :] = tail
        block = turn[:LANE, :].T
        for g, (b, j) in enumerate(groups):
            flat[bins + b, 0, pl.ds(j, SUB, stride=tall), :] = block[g * SUB : (g + 1) * SUB]
        for b in range(bins):
            deposit[b] = flat[bins + b, 0][:, :chunk]

    for b in range(bins):
        meridional(HSUB, b, keep_last)

    written = [
        pltpu.make_async_copy(flat.at[b, v], out.at[b, :, pl.ds(v * LANE, LANE)], out_sem.at[0])
        for v in range(wide)
        for b in range(bins)
    ]
    with scope("gather"):
        for v in range(wide):
            block = jnp.concatenate(
                [q3[b, v * tall + j] for b, j in groups] + [jnp.zeros((LANE - bins * rows, LANE), jnp.float32)], axis=0
            )
            turn[pl.ds(v, LANE, stride=wide), :] = block.T
        for v in range(wide):
            block = turn[v * LANE : (v + 1) * LANE, :].T
            for g, (b, j) in enumerate(groups):
                flat[b, v, pl.ds(j, SUB, stride=tall), :] = block[g * SUB : (g + 1) * SUB]
            for copy in written[v * bins : (v + 1) * bins]:
                copy.start()

    with scope("sent"):
        @pl.when(has_north)
        def _():
            north_row.wait_send()

        for side, there in ((0, has_north), (1, has_south)):
            @pl.when(there)
            def _():
                pltpu.make_async_remote_copy(
                    hs.at[side], hr.at[side], hs_sem.at[side], hr_sem.at[0, side, 0],
                    device_id={"lat": band + 1 if side == 0 else band - 1}, device_id_type=MESH,
                ).wait_send()

        all_fall.wait_send()
        for b in range(bins):
            holder(b, w_sem, 0)
            settler(b, b_sem, 0)
        all_drops.wait_send()
    with scope("written"):
        pltpu.make_async_copy(flat.at[pl.ds(0, bins)], flat.at[pl.ds(0, bins)], out_sem.at[0]).wait()


def on_device(bands, levels, tracer, east, north, fall):
    bins, _, rows, width = tracer.shape
    tall, wide = rows // SUB, width // LANE
    chunk = width // levels
    main = tall * (wide - 1) // levels
    each = main + 1
    share = main * bins + (1 if bins * tall <= levels else bins)
    edge = -(-3 * wide // SUB) * SUB
    line = -(-wide // SUB) * SUB
    steps = HSUB + 1
    f32 = jnp.float32
    field = VMEM((bins, wide * tall, SUB, LANE), f32)
    dealt = VMEM((bins, levels * each, SUB, LANE), f32)
    columns = VMEM((bins, levels, each, SUB, LANE), f32)
    out, deposit = pl.pallas_call(
        functools.partial(kernel, bands, levels),
        out_shape=(
            jax.ShapeDtypeStruct((bins, rows, width), f32),
            jax.ShapeDtypeStruct((bins, rows, chunk), f32),
        ),
        in_specs=[pl.BlockSpec(memory_space=pltpu.HBM)] * 4,
        out_specs=(pl.BlockSpec(memory_space=pltpu.HBM), pl.BlockSpec(memory_space=VMEM)),
        scratch_shapes=[
            VMEM((2 + 2 * bins, wide, rows, LANE), f32),
            VMEM((width, LANE), f32),
            dealt,
            field,
            dealt,
            field,
            VMEM((levels * share, SUB, LANE), f32),
            VMEM((3, tall, wide + 1, SUB, LANE), f32),
            VMEM((3, wide, tall + 1, SUB, LANE), f32),
            VMEM((2, steps, bins, edge, LANE), f32),
            VMEM((2, steps, bins, edge, LANE), f32),
            VMEM((line, LANE), f32),
            VMEM((line, LANE), f32),
            VMEM((levels, share, SUB, LANE), f32),
            columns,
            columns,
            VMEM((LANE, LANE), f32),
            VMEM((LANE, LANE), f32),
            VMEM((levels, LANE // levels, LANE), f32),
            DMA((2 + 2 * bins,)),
            DMA((1,)),
            DMA((2,)),
            DMA((2, 2, bins)),
            DMA((2,)),
            DMA((2,)),
            DMA((2, bins)),
            DMA((2, bins)),
            DMA((2,)),
        ],
        compiler_params=pltpu.CompilerParams(collective_id=0, has_side_effects=True),
        cost_estimate=pl.CostEstimate(flops=50000000, bytes_accessed=3000000, transcendentals=700000),
    )(
        tracer.reshape(bins, rows, width),
        east.reshape(rows, width),
        north.reshape(rows, width),
        fall.reshape(bins, rows, width),
    )
    return out.reshape(tracer.shape), deposit


def solution(mesh):
    in_specs = (
        P(None, "lev", "lat", None),
        P("lev", "lat", None),
        P("lev", "lat", None),
        P(None, "lev", "lat", None),
    )
    out_specs = (P(None, "lev", "lat", None), P(None, "lat", "lev"))
    return jax.shard_map(
        functools.partial(on_device, mesh.shape["lat"], mesh.shape["lev"]),
        mesh=mesh, in_specs=in_specs, out_specs=out_specs, check_vma=False,
    )
```

```python
import functools

import jax
import jax.numpy as jnp
from jax import lax
from jax.experimental import pallas as pl
from jax.experimental.pallas import tpu as pltpu
from jax.sharding import PartitionSpec as P

HSUB = 4
SETTLE_SUBSTEPS = 6
SUB = 8
LANE = 128
MESH = pl.DeviceIdType.MESH
VMEM = pltpu.VMEM
DMA = pltpu.SemaphoreType.DMA
scope = jax.named_scope


def coefficients(k):
    s = jnp.abs(k)
    half = 0.5 * k * s
    a3 = 3.0 * half * (1.0 - (2.0 / 3.0) * s)
    return k - a3 - half, 2.0 * a3, half - a3


def swept(ext, c0, c1, c2):
    n = ext.shape[0] - 6
    b, c = ext[1 : n + 4], ext[2 : n + 5]
    face = (7.0 / 12.0) * (b + c) - (1.0 / 12.0) * (ext[: n + 3] + ext[3:])
    face = jnp.minimum(jnp.maximum(face, jnp.minimum(b, c)), jnp.maximum(b, c))
    up = c1 >= 0
    flux = (
        c0 * face[1 : n + 2]
        + c1 * jnp.where(up, ext[2 : n + 3], ext[3 : n + 4])
        + c2 * jnp.where(up, face[: n + 1], face[2:])
    )
    return ext[3 : n + 3] - (flux[1:] - flux[:-1])


def kernel(
    bands, levels,
    tracer, east, north, fall, out, deposit,
    flat, turn, q, z, q2, q3, fs, cz, czp, cm, p, zp, hs, hr, hsf, hrf, cs, cr, pe, rf, rw, so, dblk, dts, dr,
    in_sem, out_sem, hs_sem, hr_sem, c_sem, f_sem, w_sem, b_sem, d_sem,
):
    bins, rows, width = tracer.shape
    tall = rows // SUB
    wide = width // LANE
    main = tall * (wide - 1) // levels
    each = main + 1
    spare = 1 if bins * tall <= levels else bins
    share = main * bins + spare
    across = levels // 4
    lanes_each = LANE // levels
    chunk = width // levels
    groups = [(b, j) for b in range(bins) for j in range(tall)]
    band = lax.axis_index("lat")
    me = lax.axis_index("lev")
    has_south, has_north = band > 0, band < bands - 1
    sub = lax.broadcasted_iota(jnp.int32, (SUB, LANE), 0)
    first, last = sub == 0, sub == SUB - 1

    half_at, x_at, core_at = me // (2 * across), lax.rem(me // 2, across), lax.rem(me, 2)
    moves = [
        (h, x, c)
        for h in (1, 0)
        for x in sorted(range(across), key=lambda x: -min(x, across - x))
        for c in range(2)
        if (h, x, c) != (0, 0, 0)
    ]
    n_moves = len(moves)
    same_half = [i for i, m in enumerate(moves) if m[0] == 0]
    other_half = [i for i, m in enumerate(moves) if m[0] == 1]

    def at(h, x, c):
        return (lax.rem(half_at + h, 2) * across + lax.rem(x_at + x, across)) * 2 + lax.rem(core_at + c, 2)

    def to(i):
        return at(*moves[i])

    def origin(i):
        h, x, c = moves[i]
        return at(h, across - x, c)

    barrier = pltpu.get_barrier_semaphore()
    for i in range(n_moves):
        pl.semaphore_signal(barrier, inc=1, device_id={"lev": to(i)}, device_id_type=MESH)

    @pl.when(has_south)
    def _():
        pl.semaphore_signal(barrier, inc=1, device_id={"lat": band - 1}, device_id_type=MESH)

    @pl.when(has_north)
    def _():
        pl.semaphore_signal(barrier, inc=1, device_id={"lat": band + 1}, device_id_type=MESH)

    def fetch(source, slot):
        return [
            pltpu.make_async_copy(
                source.at[:, pl.ds(v * LANE, LANE)], flat.at[slot, v], in_sem.at[slot]
            )
            for v in range(wide)
        ]

    fetched = [fetch(tracer.at[b], b) for b in range(bins)] + [fetch(east, bins), fetch(north, bins + 1)]
    fetched += [fetch(fall.at[b], bins + 2 + b) for b in range(bins)]
    for copies in fetched:
        for copy in copies:
            copy.start()

    for side, beyond in ((0, band == 0), (1, band == bands - 1)):
        @pl.when(beyond)
        def _():
            cr[side] = jnp.zeros(cr.shape[1:], jnp.float32)
            for b in range(bins):
                hrf[side, b] = jnp.zeros(hrf.shape[2:], jnp.float32)
                for e in range(2):
                    hr[side, e, b] = jnp.zeros(hr.shape[3:], jnp.float32)

    dblk[...] = jnp.zeros_like(dblk)

    def spread(slot, emit):
        for i in range(2):
            pltpu.make_async_copy(flat.at[slot + i], flat.at[slot + i], in_sem.at[slot + i]).wait()
        for v in range(wide):
            block = jnp.concatenate(
                [flat[slot + i, v, pl.ds(j, SUB, stride=tall), :] for i in range(2) for j in range(tall)]
                + [jnp.zeros((LANE - 2 * rows, LANE), jnp.float32)],
                axis=0,
            )
            turn[v * LANE : (v + 1) * LANE, :] = block.T
        for v in range(wide):
            block = turn[pl.ds(v, LANE, stride=wide), :].T
            for i in range(2):
                for j in range(tall):
                    start = (i * tall + j) * SUB
                    emit(i, j, v, block[start : start + SUB])

    def owner(b, j):
        half_tall = tall // 2
        return (tall * b + 2 * (j % half_tall) + (1 if j < half_tall else 0)) % levels

    def extra(b, t):
        u = lax.rem(t + levels * bins - tall * b, levels)
        return u < tall, u // 2 + (tall // 2) * (1 - lax.rem(u, 2))

    def place(b, v, j):
        tile = v * tall + j
        return (tile // main, tile % main) if v < wide - 1 else (owner(b, j), main)

    def index(b, v, j):
        t, i = place(b, v, j)
        return t * each + i

    def emit_tracer(b, j, v, tile):
        q[b, index(b, v, j)] = tile

    def emit_courant(i, j, v, tile):
        if i == 1 and j == tall - 1:
            tile = jnp.where(jnp.logical_and(last, band == bands - 1), 0.0, tile)
        sent, at_row = (3, 4) if i == 0 else (4, 0)
        if j >= tall - sent:
            cs[0, pl.ds((at_row + j - tall + sent) * wide + v, 1), :] = tile[SUB - 1 :, :]
        if j < 3:
            cs[1, pl.ds((at_row + j) * wide + v, 1), :] = tile[:1, :]
        for n, c in enumerate(coefficients(tile)):
            if i == 0:
                cz[n, j, v + 1] = c
            else:
                cm[n, v, j + 4] = c

    def emit_fall(b, j, v, tile):
        t, i = place(b, v, j)
        fs[t * share + (b * main + i if i < main else bins * main + b % spare)] = tile

    with scope("spread"):
        spread(0, emit_tracer)
        spread(bins, emit_courant)
        for n in range(3):
            for j in range(tall):
                cz[n, j, 0] = pltpu.roll(cz[n, j, wide], 1, 1)

    def near(side):
        return {"lat": band + 1 if side == 0 else band - 1}

    def courants(side):
        return pltpu.make_async_remote_copy(
            cs.at[side], cr.at[side], c_sem.at[0, side], c_sem.at[1, side], device_id=near(side), device_id_type=MESH
        )

    def halo(e, side, b):
        source, target = (hs.at[side, e, b], hr.at[side, e, b]) if e < 2 else (hsf.at[side, b], hrf.at[side, b])
        return pltpu.make_async_remote_copy(
            source, target, hs_sem.at[e // 2, side], hr_sem.at[e, side, b], device_id=near(side), device_id_type=MESH
        )

    def zonal_row(own, c0, c1, c2):
        ext = [pltpu.roll(t, 1, 1) for t in own[-3:]] + own + [pltpu.roll(t, LANE - 1, 1) for t in own[:3]]
        return swept(jnp.stack(ext), c0, c1, c2)

    def zonal(e, b, field):
        with scope("zonal"):
            for j in range(tall):
                new = zonal_row([field[b, index(b, v, j)] for v in range(wide)], cz[0, j], cz[1, j], cz[2, j])
                for v in range(wide):
                    z[b, v * tall + j] = new[v]
                    low, high = new[v][:1, :], new[v][SUB - 1 :, :]
                    if e in (0, 1):
                        hs[1, e, b, pl.ds(j * wide + v, 1), :] = low
                        hs[0, e, b, pl.ds(j * wide + v, 1), :] = high
                    elif e == 2 and j < 3:
                        hsf[1, b, pl.ds(j * wide + v, 1), :] = low
                    elif e == 2 and j >= tall - 3:
                        hsf[0, b, pl.ds((j - tall + 3) * wide + v, 1), :] = high
            if e is None:
                new = zonal_row([p[b, v] for v in range(wide)], czp[0], czp[1], czp[2])
                for v in range(wide):
                    zp[b, v] = new[v]

    def send_halo(e, b):
        @pl.when(has_north)
        def _():
            halo(e, 0, b).start()

        @pl.when(has_south)
        def _():
            halo(e, 1, b).start()

    def wait_halo(e, b):
        with scope("halo"):
            @pl.when(has_south)
            def _():
                halo(e, 0, b).wait_recv()

            @pl.when(has_north)
            def _():
                halo(e, 1, b).wait_recv()

    def extended(own, lows, highs):
        n = len(lows)
        below = [jnp.where(first, lows[i], pltpu.roll(own[tall - n + i], 1, 0)) for i in range(n)]
        above = [jnp.where(last, highs[i], pltpu.roll(own[i], SUB - 1, 0)) for i in range(n)]
        return jnp.stack(below + own + above)

    def meridional_wide(e, b):
        wait_halo(e, b)
        with scope("meridional_wide"):
            for v in range(wide):
                own = [z[b, v * tall + j] for j in range(tall)]
                lows = [hr[0, e, b, pl.ds(i * wide + v, 1), :] for i in range(tall)]
                highs = [hr[1, e, b, pl.ds(i * wide + v, 1), :] for i in range(tall)]
                new = swept(extended(own, lows, highs), cm[0, v], cm[1, v], cm[2, v])
                for j in range(tall):
                    q[b, index(b, v, j)] = new[j + 3]
                for i in range(3):
                    p[b, v, i : i + 1, :] = new[i][:1, :]
                    p[b, v, i + 3 : i + 4, :] = new[tall + 3 + i][SUB - 1 :, :]

    def meridional(b, rows_of, keep):
        with scope("meridional"):
            for v in range(wide):
                own = [z[b, v * tall + j] for j in range(tall)]
                lows, highs = rows_of(b, v)
                c0, c1, c2 = [cm[n, v, 3 : tall + 4] for n in range(3)]
                new = swept(extended(own, lows, highs), c0, c1, c2)
                for j in range(tall):
                    keep(b, v, j, new[j])

    def rows_kept(b, v):
        return [zp[b, v, i : i + 1, :] for i in range(3)], [zp[b, v, i + 3 : i + 4, :] for i in range(3)]

    def rows_sent(b, v):
        return [[hrf[side, b, pl.ds(i * wide + v, 1), :] for i in range(3)] for side in range(2)]

    def keep_mass(b, v, j, tile):
        q[b, index(b, v, j)] = tile

    def keep_last(b, v, j, tile):
        q3[b, v * tall + j] = tile

    def copy_to(i, source, target, send, recv):
        return pltpu.make_async_remote_copy(
            source, target, send, recv, device_id={"lev": to(i)}, device_id_type=MESH
        )

    def either(condition, yes, no):
        @pl.when(condition)
        def _():
            yes()

        @pl.when(jnp.logical_not(condition))
        def _():
            no()

    def deal_fall(i):
        return copy_to(i, fs.at[pl.ds(to(i) * share, share)], rf.at[me], f_sem.at[0], f_sem.at[1])

    def deal_mass(b, i):
        t = to(i)
        send, recv = w_sem.at[0, b], w_sem.at[1, b]
        either(
            extra(b, t)[0],
            copy_to(i, q.at[b, pl.ds(t * each, each)], rw.at[b, me], send, recv).start,
            copy_to(i, q.at[b, pl.ds(t * each, main)], rw.at[b, me, pl.ds(0, main)], send, recv).start,
        )

    def give_back(b, i):
        t = to(i)
        send, recv = b_sem.at[0, b], b_sem.at[1, b]
        either(
            extra(b, me)[0],
            copy_to(i, so.at[b, t], q2.at[b, pl.ds(me * each, each)], send, recv).start,
            copy_to(i, so.at[b, t, pl.ds(0, main)], q2.at[b, pl.ds(me * each, main)], send, recv).start,
        )

    def settler(b, sems, side):
        full, part = rw.at[b, pl.ds(0, n_moves)], rw.at[b, pl.ds(0, n_moves), pl.ds(0, main)]
        name = "wait_recv" if side else "wait_send"
        either(
            extra(b, me)[0],
            getattr(copy_to(0, full, full, sems.at[0, b], sems.at[1, b]), name),
            getattr(copy_to(0, part, part, sems.at[0, b], sems.at[1, b]), name),
        )

    def holder(b, sems, side):
        count = n_moves * main + tall
        few, many = q.at[b, pl.ds(0, count - 1)], q.at[b, pl.ds(0, count)]
        name = "wait_recv" if side else "wait_send"
        either(
            extra(b, me)[0],
            getattr(copy_to(0, few, few, sems.at[0, b], sems.at[1, b]), name),
            getattr(copy_to(0, many, many, sems.at[0, b], sems.at[1, b]), name),
        )

    all_fall = copy_to(0, rf.at[pl.ds(0, n_moves)], rf.at[pl.ds(0, n_moves)], f_sem.at[0], f_sem.at[1])

    def send_fall(some):
        for i in some:
            deal_fall(i).start()

    for b in range(bins):
        p[b] = jnp.zeros(p.shape[1:], jnp.float32)
    pe[...] = jnp.zeros_like(pe)
    for b in range(bins):
        zonal(0, b, q)
    with scope("spread_fall"):
        spread(bins + 2, emit_fall)
    with scope("barrier"):
        pl.semaphore_wait(barrier, n_moves + has_south.astype(jnp.int32) + has_north.astype(jnp.int32))

    @pl.when(has_north)
    def _():
        courants(0).start()

    @pl.when(has_south)
    def _():
        courants(1).start()

    for b in range(bins):
        send_halo(0, b)
    with scope("send_fall"):
        send_fall(same_half + other_half)
    for i in range(share):
        rf[me, i] = fs[me * share + i]

    with scope("courants"):
        @pl.when(has_south)
        def _():
            courants(0).wait_recv()

        @pl.when(has_north)
        def _():
            courants(1).wait_recv()

    with scope("edge_coefficients"):
        for v in range(wide):
            for i in range(4):
                low = coefficients(cr[0, pl.ds(i * wide + v, 1), :])
                for n in range(3):
                    cm[n, v, i] = jnp.where(first, low[n], pltpu.roll(cm[n, v, i + tall], 1, 0))
            for i in range(3):
                high = coefficients(cr[1, pl.ds(i * wide + v, 1), :])
                for n in range(3):
                    cm[n, v, tall + 4 + i] = jnp.where(last, high[n], pltpu.roll(cm[n, v, i + 4], SUB - 1, 0))
                pe[v, i : i + 1, :] = cr[0, pl.ds((4 + i) * wide + v, 1), :]
                pe[v, i + 3 : i + 4, :] = cr[1, pl.ds((4 + i) * wide + v, 1), :]
        for v in range(wide):
            for n, c in enumerate(coefficients(pe[v])):
                czp[n, v + 1] = c
        for n in range(3):
            czp[n, 0] = pltpu.roll(czp[n, wide], 1, 1)

    for e in range(HSUB // 2):
        if e:
            for b in range(bins):
                zonal(e, b, q)
                send_halo(e, b)
        for b in range(bins):
            meridional_wide(e, b)
            zonal(None, b, q)
            meridional(b, rows_kept, keep_mass)
            if e == HSUB // 2 - 1:
                for i in range(n_moves):
                    deal_mass(b, i)

    for b in range(bins):
        owned, extra_j = extra(b, me)
        for i in range(main):
            rw[b, me, i] = q[b, me * each + i]

        @pl.when(owned)
        def _():
            rw[b, me, main] = q[b, me * each + main]

        if b == 0:
            with scope("wait_fall"):
                all_fall.wait_recv()
        with scope("wait_mass"):
            settler(b, w_sem, 1)

        def settle(i, j):
            mass = rw[b, :, i]
            half = 0.5 * rf[:, b * main + i if i < main else bins * main + b % spare]
            fallen = jnp.zeros((SUB, LANE), jnp.float32)
            for _ in range(SETTLE_SUBSTEPS):
                flux = (mass * half) * (2.0 + jnp.tanh(mass))
                inflow = jnp.concatenate([jnp.zeros((1, SUB, LANE), jnp.float32), flux[:-1]], axis=0)
                mass = (mass + inflow) - flux
                fallen = fallen + flux[levels - 1]
            so[b, :, i] = mass
            dblk[pl.ds((b * tall + j) * SUB, SUB), :] = fallen

        with scope("settle"):
            for i in range(main):
                settle(i, lax.rem(me * main + i, tall))

            @pl.when(owned)
            def _():
                settle(main, extra_j)

        with scope("give_back"):
            for i in range(n_moves):
                give_back(b, i)
        for i in range(main):
            q2[b, me * each + i] = so[b, me, i]

        @pl.when(owned)
        def _():
            q2[b, me * each + main] = so[b, me, main]

    dts[...] = dblk[...].T

    def drop(i):
        return pltpu.make_async_remote_copy(
            dts.at[pl.ds(to(i) * lanes_each, lanes_each)], dr.at[me], d_sem.at[0], d_sem.at[1],
            device_id={"lev": to(i)}, device_id_type=MESH,
        )

    for i in range(n_moves):
        drop(i).start()
    dr[me] = dts[pl.ds(me * lanes_each, lanes_each), :]

    for b in range(bins):
        with scope("wait_back"):
            holder(b, b_sem, 1)
        zonal(2, b, q2)
        send_halo(2, b)

    with scope("deposit"):
        all_drops = copy_to(0, dr.at[pl.ds(0, n_moves)], dr.at[pl.ds(0, n_moves)], d_sem.at[0], d_sem.at[1])
        all_drops.wait_recv()
        column = lax.broadcasted_iota(jnp.int32, (lanes_each, LANE), 1) // SUB
        low_rows = lax.rem(column, tall) < tall // 2
        for v in range(wide - 1):
            turn[pl.ds(v, lanes_each, stride=wide), :] = jnp.where(low_rows, dr[2 * v], dr[2 * v + 1])
        tail = jnp.zeros((lanes_each, LANE), jnp.float32)
        for g, (b, j) in enumerate(groups):
            t = (tall * b + 2 * (j % (tall // 2)) + (1 if j < tall // 2 else 0)) % levels
            tail = jnp.where(column == g, dr[t], tail)
        turn[pl.ds(wide - 1, lanes_each, stride=wide), :] = tail
        block = turn[:LANE, :].T
        for g, (b, j) in enumerate(groups):
            flat[bins + b, 0, pl.ds(j, SUB, stride=tall), :] = block[g * SUB : (g + 1) * SUB]
        for b in range(bins):
            deposit[b] = flat[bins + b, 0][:, :chunk]

    for b in range(bins):
        wait_halo(2, b)
        meridional(b, rows_sent, keep_last)

    written = [
        pltpu.make_async_copy(flat.at[b, v], out.at[b, :, pl.ds(v * LANE, LANE)], out_sem.at[0])
        for v in range(wide)
        for b in range(bins)
    ]
    with scope("gather"):
        for v in range(wide):
            block = jnp.concatenate(
                [q3[b, v * tall + j] for b, j in groups] + [jnp.zeros((LANE - bins * rows, LANE), jnp.float32)], axis=0
            )
            turn[pl.ds(v, LANE, stride=wide), :] = block.T
        for v in range(wide):
            block = turn[v * LANE : (v + 1) * LANE, :].T
            for g, (b, j) in enumerate(groups):
                flat[b, v, pl.ds(j, SUB, stride=tall), :] = block[g * SUB : (g + 1) * SUB]
            for copy in written[v * bins : (v + 1) * bins]:
                copy.start()

    with scope("sent"):
        for side, there in ((0, has_north), (1, has_south)):
            @pl.when(there)
            def _():
                courants(side).wait_send()
                for kind, (source, target) in enumerate(((hs, hr), (hsf, hrf))):
                    pltpu.make_async_remote_copy(
                        source.at[side], target.at[side], hs_sem.at[kind, side], hr_sem.at[0, side, 0],
                        device_id=near(side), device_id_type=MESH,
                    ).wait_send()

        all_fall.wait_send()
        for b in range(bins):
            holder(b, w_sem, 0)
            settler(b, b_sem, 0)
        all_drops.wait_send()
    with scope("written"):
        pltpu.make_async_copy(flat.at[pl.ds(0, bins)], flat.at[pl.ds(0, bins)], out_sem.at[0]).wait()


def on_device(bands, levels, tracer, east, north, fall):
    bins, _, rows, width = tracer.shape
    tall, wide = rows // SUB, width // LANE
    chunk = width // levels
    main = tall * (wide - 1) // levels
    each = main + 1
    share = main * bins + (1 if bins * tall <= levels else bins)
    def lines(n):
        return -(-n * wide // SUB) * SUB

    f32 = jnp.float32
    field = VMEM((bins, wide * tall, SUB, LANE), f32)
    dealt = VMEM((bins, levels * each, SUB, LANE), f32)
    columns = VMEM((bins, levels, each, SUB, LANE), f32)
    out, deposit = pl.pallas_call(
        functools.partial(kernel, bands, levels),
        out_shape=(
            jax.ShapeDtypeStruct((bins, rows, width), f32),
            jax.ShapeDtypeStruct((bins, rows, chunk), f32),
        ),
        in_specs=[pl.BlockSpec(memory_space=pltpu.HBM)] * 4,
        out_specs=(pl.BlockSpec(memory_space=pltpu.HBM), pl.BlockSpec(memory_space=VMEM)),
        scratch_shapes=[
            VMEM((2 + 2 * bins, wide, rows, LANE), f32),
            VMEM((width, LANE), f32),
            dealt,
            field,
            dealt,
            field,
            VMEM((levels * share, SUB, LANE), f32),
            VMEM((3, tall, wide + 1, SUB, LANE), f32),
            VMEM((3, wide + 1, SUB, LANE), f32),
            VMEM((3, wide, tall + 7, SUB, LANE), f32),
            VMEM((bins, wide, SUB, LANE), f32),
            VMEM((bins, wide, SUB, LANE), f32),
            VMEM((2, 2, bins, lines(tall), LANE), f32),
            VMEM((2, 2, bins, lines(tall), LANE), f32),
            VMEM((2, bins, lines(3), LANE), f32),
            VMEM((2, bins, lines(3), LANE), f32),
            VMEM((2, lines(7), LANE), f32),
            VMEM((2, lines(7), LANE), f32),
            VMEM((wide, SUB, LANE), f32),
            VMEM((levels, share, SUB, LANE), f32),
            columns,
            columns,
            VMEM((LANE, LANE), f32),
            VMEM((LANE, LANE), f32),
            VMEM((levels, LANE // levels, LANE), f32),
            DMA((2 + 2 * bins,)),
            DMA((1,)),
            DMA((2, 2)),
            DMA((3, 2, bins)),
            DMA((2, 2)),
            DMA((2,)),
            DMA((2, bins)),
            DMA((2, bins)),
            DMA((2,)),
        ],
        compiler_params=pltpu.CompilerParams(collective_id=0, has_side_effects=True),
        cost_estimate=pl.CostEstimate(flops=50000000, bytes_accessed=3000000, transcendentals=700000),
    )(
        tracer.reshape(bins, rows, width),
        east.reshape(rows, width),
        north.reshape(rows, width),
        fall.reshape(bins, rows, width),
    )
    return out.reshape(tracer.shape), deposit


def solution(mesh):
    in_specs = (
        P(None, "lev", "lat", None),
        P("lev", "lat", None),
        P("lev", "lat", None),
        P(None, "lev", "lat", None),
    )
    out_specs = (P(None, "lev", "lat", None), P(None, "lat", "lev"))
    return jax.shard_map(
        functools.partial(on_device, mesh.shape["lat"], mesh.shape["lev"]),
        mesh=mesh, in_specs=in_specs, out_specs=out_specs, check_vma=False,
    )
```

```python
import functools

import jax
import jax.numpy as jnp
from jax import lax
from jax.experimental import pallas as pl
from jax.experimental.pallas import tpu as pltpu
from jax.sharding import PartitionSpec as P

HSUB = 4
SETTLE_SUBSTEPS = 6
SUB = 8
LANE = 128
MESH = pl.DeviceIdType.MESH
VMEM = pltpu.VMEM
DMA = pltpu.SemaphoreType.DMA
scope = jax.named_scope


def coefficients(k):
    s = jnp.abs(k)
    half = 0.5 * k * s
    a3 = 3.0 * half * (1.0 - (2.0 / 3.0) * s)
    return k - a3 - half, 2.0 * a3, half - a3


def swept(ext, c0, c1, c2):
    n = ext.shape[0] - 6
    b, c = ext[1 : n + 4], ext[2 : n + 5]
    face = (7.0 / 12.0) * (b + c) - (1.0 / 12.0) * (ext[: n + 3] + ext[3:])
    face = jnp.minimum(jnp.maximum(face, jnp.minimum(b, c)), jnp.maximum(b, c))
    up = c1 >= 0
    flux = (
        c0 * face[1 : n + 2]
        + c1 * jnp.where(up, ext[2 : n + 3], ext[3 : n + 4])
        + c2 * jnp.where(up, face[: n + 1], face[2:])
    )
    return ext[3 : n + 3] - (flux[1:] - flux[:-1])


def kernel(
    bands, levels,
    tracer, east, north, fall, out, deposit,
    flat, turn, q, z, q2, q3, fs, cz, czp, cm, p, zp, hs, hr, hsf, hrf, cs, cr, pe, rf, rw, so, dblk, dts, dr,
    in_sem, hs_sem, hr_sem, c_sem, f_sem, w_sem, b_sem, d_sem,
):
    bins, rows, width = tracer.shape
    tall = rows // SUB
    wide = width // LANE
    main = tall * (wide - 1) // levels
    each = main + 1
    spare = 1 if bins * tall <= levels else bins
    share = main * bins + spare
    across = levels // 4
    lanes_each = LANE // levels
    chunk = width // levels
    groups = [(b, j) for b in range(bins) for j in range(tall)]
    band = lax.axis_index("lat")
    me = lax.axis_index("lev")
    has_south, has_north = band > 0, band < bands - 1
    sub = lax.broadcasted_iota(jnp.int32, (SUB, LANE), 0)
    first, last = sub == 0, sub == SUB - 1

    half_at, x_at, core_at = me // (2 * across), lax.rem(me // 2, across), lax.rem(me, 2)
    moves = [
        (h, x, c)
        for h in (1, 0)
        for x in sorted(range(across), key=lambda x: -min(x, across - x))
        for c in range(2)
        if (h, x, c) != (0, 0, 0)
    ]
    n_moves = len(moves)
    same_half = [i for i, m in enumerate(moves) if m[0] == 0]
    other_half = [i for i, m in enumerate(moves) if m[0] == 1]

    def at(h, x, c):
        return (lax.rem(half_at + h, 2) * across + lax.rem(x_at + x, across)) * 2 + lax.rem(core_at + c, 2)

    def to(i):
        return at(*moves[i])

    def origin(i):
        h, x, c = moves[i]
        return at(h, across - x, c)

    barrier = pltpu.get_barrier_semaphore()
    for i in range(n_moves):
        pl.semaphore_signal(barrier, inc=1, device_id={"lev": to(i)}, device_id_type=MESH)

    @pl.when(has_south)
    def _():
        pl.semaphore_signal(barrier, inc=1, device_id={"lat": band - 1}, device_id_type=MESH)

    @pl.when(has_north)
    def _():
        pl.semaphore_signal(barrier, inc=1, device_id={"lat": band + 1}, device_id_type=MESH)

    def fetch(source, slot):
        return [
            pltpu.make_async_copy(
                source.at[:, pl.ds(v * LANE, LANE)], flat.at[slot, v], in_sem.at[slot]
            )
            for v in range(wide)
        ]

    fetched = [fetch(tracer.at[b], b) for b in range(bins)] + [fetch(east, bins), fetch(north, bins + 1)]
    fetched += [fetch(fall.at[b], bins + 2 + b) for b in range(bins)]
    for copies in fetched:
        for copy in copies:
            copy.start()

    for side, beyond in ((0, band == 0), (1, band == bands - 1)):
        @pl.when(beyond)
        def _():
            cr[side] = jnp.zeros(cr.shape[1:], jnp.float32)
            for b in range(bins):
                hrf[side, b] = jnp.zeros(hrf.shape[2:], jnp.float32)
                for e in range(2):
                    hr[side, e, b] = jnp.zeros(hr.shape[3:], jnp.float32)

    dblk[...] = jnp.zeros_like(dblk)

    def spread(slot, emit):
        for i in range(2):
            pltpu.make_async_copy(flat.at[slot + i], flat.at[slot + i], in_sem.at[slot + i]).wait()
        for v in range(wide):
            block = jnp.concatenate(
                [flat[slot + i, v, pl.ds(j, SUB, stride=tall), :] for i in range(2) for j in range(tall)]
                + [jnp.zeros((LANE - 2 * rows, LANE), jnp.float32)],
                axis=0,
            )
            turn[v * LANE : (v + 1) * LANE, :] = block.T
        for v in range(wide):
            block = turn[pl.ds(v, LANE, stride=wide), :].T
            for i in range(2):
                for j in range(tall):
                    start = (i * tall + j) * SUB
                    emit(i, j, v, block[start : start + SUB])

    def owner(b, j):
        half_tall = tall // 2
        return (tall * b + 2 * (j % half_tall) + (1 if j < half_tall else 0)) % levels

    def extra(b, t):
        u = lax.rem(t + levels * bins - tall * b, levels)
        return u < tall, u // 2 + (tall // 2) * (1 - lax.rem(u, 2))

    def place(b, v, j):
        tile = v * tall + j
        return (tile // main, tile % main) if v < wide - 1 else (owner(b, j), main)

    def index(b, v, j):
        t, i = place(b, v, j)
        return t * each + i

    def emit_tracer(b, j, v, tile):
        q[b, index(b, v, j)] = tile

    def emit_courant(i, j, v, tile):
        if i == 1 and j == tall - 1:
            tile = jnp.where(jnp.logical_and(last, band == bands - 1), 0.0, tile)
        sent, at_row = (3, 4) if i == 0 else (4, 0)
        if j >= tall - sent:
            cs[0, pl.ds((at_row + j - tall + sent) * wide + v, 1), :] = tile[SUB - 1 :, :]
        if j < 3:
            cs[1, pl.ds((at_row + j) * wide + v, 1), :] = tile[:1, :]
        for n, c in enumerate(coefficients(tile)):
            if i == 0:
                cz[n, j, v + 1] = c
            else:
                cm[n, v, j + 4] = c

    def emit_fall(b, j, v, tile):
        t, i = place(b, v, j)
        fs[t * share + (b * main + i if i < main else bins * main + b % spare)] = tile

    with scope("spread"):
        spread(0, emit_tracer)
        spread(bins, emit_courant)
        for n in range(3):
            for j in range(tall):
                cz[n, j, 0] = pltpu.roll(cz[n, j, wide], 1, 1)

    def near(side):
        return {"lat": band + 1 if side == 0 else band - 1}

    def courants(side):
        return pltpu.make_async_remote_copy(
            cs.at[side], cr.at[side], c_sem.at[0, side], c_sem.at[1, side], device_id=near(side), device_id_type=MESH
        )

    def halo(e, side, b):
        source, target = (hs.at[side, e, b], hr.at[side, e, b]) if e < 2 else (hsf.at[side, b], hrf.at[side, b])
        return pltpu.make_async_remote_copy(
            source, target, hs_sem.at[e // 2, side], hr_sem.at[e, side, b], device_id=near(side), device_id_type=MESH
        )

    def zonal_row(own, c0, c1, c2):
        ext = [pltpu.roll(t, 1, 1) for t in own[-3:]] + own + [pltpu.roll(t, LANE - 1, 1) for t in own[:3]]
        return swept(jnp.stack(ext), c0, c1, c2)

    def zonal(e, b, field):
        with scope("zonal"):
            for j in range(tall):
                new = zonal_row([field[b, index(b, v, j)] for v in range(wide)], cz[0, j], cz[1, j], cz[2, j])
                for v in range(wide):
                    z[b, v * tall + j] = new[v]
                    low, high = new[v][:1, :], new[v][SUB - 1 :, :]
                    if e in (0, 1):
                        hs[1, e, b, pl.ds(j * wide + v, 1), :] = low
                        hs[0, e, b, pl.ds(j * wide + v, 1), :] = high
                    elif e == 2 and j < 3:
                        hsf[1, b, pl.ds(j * wide + v, 1), :] = low
                    elif e == 2 and j >= tall - 3:
                        hsf[0, b, pl.ds((j - tall + 3) * wide + v, 1), :] = high
            if e is None:
                new = zonal_row([p[b, v] for v in range(wide)], czp[0], czp[1], czp[2])
                for v in range(wide):
                    zp[b, v] = new[v]

    def send_halo(e, b):
        @pl.when(has_north)
        def _():
            halo(e, 0, b).start()

        @pl.when(has_south)
        def _():
            halo(e, 1, b).start()

    def wait_halo(e, b):
        with scope("halo"):
            @pl.when(has_south)
            def _():
                halo(e, 0, b).wait_recv()

            @pl.when(has_north)
            def _():
                halo(e, 1, b).wait_recv()

    def extended(own, lows, highs):
        n = len(lows)
        below = [jnp.where(first, lows[i], pltpu.roll(own[tall - n + i], 1, 0)) for i in range(n)]
        above = [jnp.where(last, highs[i], pltpu.roll(own[i], SUB - 1, 0)) for i in range(n)]
        return jnp.stack(below + own + above)

    def meridional_wide(e, b):
        wait_halo(e, b)
        if e == 0 and b == bins - 1:
            send_fall(other_half[:3])
        with scope("meridional_wide"):
            for v in range(wide):
                own = [z[b, v * tall + j] for j in range(tall)]
                lows = [hr[0, e, b, pl.ds(i * wide + v, 1), :] for i in range(tall)]
                highs = [hr[1, e, b, pl.ds(i * wide + v, 1), :] for i in range(tall)]
                new = swept(extended(own, lows, highs), cm[0, v], cm[1, v], cm[2, v])
                for j in range(tall):
                    q[b, index(b, v, j)] = new[j + 3]
                for i in range(3):
                    p[b, v, i : i + 1, :] = new[i][:1, :]
                    p[b, v, i + 3 : i + 4, :] = new[tall + 3 + i][SUB - 1 :, :]

    def meridional(b, rows_of, keep):
        with scope("meridional"):
            for v in range(wide):
                own = [z[b, v * tall + j] for j in range(tall)]
                lows, highs = rows_of(b, v)
                c0, c1, c2 = [cm[n, v, 3 : tall + 4] for n in range(3)]
                new = swept(extended(own, lows, highs), c0, c1, c2)
                for j in range(tall):
                    keep(b, v, j, new[j])

    def rows_kept(b, v):
        return [zp[b, v, i : i + 1, :] for i in range(3)], [zp[b, v, i + 3 : i + 4, :] for i in range(3)]

    def rows_sent(b, v):
        return [[hrf[side, b, pl.ds(i * wide + v, 1), :] for i in range(3)] for side in range(2)]

    def keep_mass(b, v, j, tile):
        q[b, index(b, v, j)] = tile

    def keep_last(b, v, j, tile):
        q3[b, v * tall + j] = tile

    def copy_to(i, source, target, send, recv):
        return pltpu.make_async_remote_copy(
            source, target, send, recv, device_id={"lev": to(i)}, device_id_type=MESH
        )

    def either(condition, yes, no):
        @pl.when(condition)
        def _():
            yes()

        @pl.when(jnp.logical_not(condition))
        def _():
            no()

    def deal_fall(i):
        return copy_to(i, fs.at[pl.ds(to(i) * share, share)], rf.at[me], f_sem.at[0], f_sem.at[1])

    def deal_mass(b, i):
        t = to(i)
        send, recv = w_sem.at[0, b], w_sem.at[1, b]
        either(
            extra(b, t)[0],
            copy_to(i, q.at[b, pl.ds(t * each, each)], rw.at[b, me], send, recv).start,
            copy_to(i, q.at[b, pl.ds(t * each, main)], rw.at[b, me, pl.ds(0, main)], send, recv).start,
        )

    def give_back(b, i):
        t = to(i)
        send, recv = b_sem.at[0, b], b_sem.at[1, b]
        either(
            extra(b, me)[0],
            copy_to(i, so.at[b, t], q2.at[b, pl.ds(me * each, each)], send, recv).start,
            copy_to(i, so.at[b, t, pl.ds(0, main)], q2.at[b, pl.ds(me * each, main)], send, recv).start,
        )

    def settler(b, sems, side):
        full, part = rw.at[b, pl.ds(0, n_moves)], rw.at[b, pl.ds(0, n_moves), pl.ds(0, main)]
        name = "wait_recv" if side else "wait_send"
        either(
            extra(b, me)[0],
            getattr(copy_to(0, full, full, sems.at[0, b], sems.at[1, b]), name),
            getattr(copy_to(0, part, part, sems.at[0, b], sems.at[1, b]), name),
        )

    def holder(b, sems, side):
        count = n_moves * main + tall
        few, many = q.at[b, pl.ds(0, count - 1)], q.at[b, pl.ds(0, count)]
        name = "wait_recv" if side else "wait_send"
        either(
            extra(b, me)[0],
            getattr(copy_to(0, few, few, sems.at[0, b], sems.at[1, b]), name),
            getattr(copy_to(0, many, many, sems.at[0, b], sems.at[1, b]), name),
        )

    all_fall = copy_to(0, rf.at[pl.ds(0, n_moves)], rf.at[pl.ds(0, n_moves)], f_sem.at[0], f_sem.at[1])

    def send_fall(some):
        for i in some:
            deal_fall(i).start()

    for b in range(bins):
        p[b] = jnp.zeros(p.shape[1:], jnp.float32)
    pe[...] = jnp.zeros_like(pe)
    for b in range(bins):
        zonal(0, b, q)
    with scope("spread_fall"):
        spread(bins + 2, emit_fall)
    with scope("barrier"):
        pl.semaphore_wait(barrier, n_moves + has_south.astype(jnp.int32) + has_north.astype(jnp.int32))

    @pl.when(has_north)
    def _():
        courants(0).start()

    @pl.when(has_south)
    def _():
        courants(1).start()

    for b in range(bins):
        send_halo(0, b)
    for i in range(share):
        rf[me, i] = fs[me * share + i]

    with scope("courants"):
        @pl.when(has_south)
        def _():
            courants(0).wait_recv()

        @pl.when(has_north)
        def _():
            courants(1).wait_recv()

    with scope("edge_coefficients"):
        for v in range(wide):
            for i in range(4):
                low = coefficients(cr[0, pl.ds(i * wide + v, 1), :])
                for n in range(3):
                    cm[n, v, i] = jnp.where(first, low[n], pltpu.roll(cm[n, v, i + tall], 1, 0))
            for i in range(3):
                high = coefficients(cr[1, pl.ds(i * wide + v, 1), :])
                for n in range(3):
                    cm[n, v, tall + 4 + i] = jnp.where(last, high[n], pltpu.roll(cm[n, v, i + 4], SUB - 1, 0))
                pe[v, i : i + 1, :] = cr[0, pl.ds((4 + i) * wide + v, 1), :]
                pe[v, i + 3 : i + 4, :] = cr[1, pl.ds((4 + i) * wide + v, 1), :]
        for v in range(wide):
            for n, c in enumerate(coefficients(pe[v])):
                czp[n, v + 1] = c
        for n in range(3):
            czp[n, 0] = pltpu.roll(czp[n, wide], 1, 1)

    for e in range(HSUB // 2):
        if e:
            for b in range(bins):
                zonal(e, b, q)
                send_halo(e, b)
            send_fall(other_half[3:] + same_half)
        for b in range(bins):
            meridional_wide(e, b)
            zonal(None, b, q)
            meridional(b, rows_kept, keep_mass)
            if e == HSUB // 2 - 1:
                for i in range(n_moves):
                    deal_mass(b, i)

    for b in range(bins):
        owned, extra_j = extra(b, me)
        for i in range(main):
            rw[b, me, i] = q[b, me * each + i]

        @pl.when(owned)
        def _():
            rw[b, me, main] = q[b, me * each + main]

        if b == 0:
            with scope("wait_fall"):
                all_fall.wait_recv()
        with scope("wait_mass"):
            settler(b, w_sem, 1)

        def settle(i, j):
            mass = rw[b, :, i]
            half = 0.5 * rf[:, b * main + i if i < main else bins * main + b % spare]
            fallen = jnp.zeros((SUB, LANE), jnp.float32)
            for _ in range(SETTLE_SUBSTEPS):
                flux = (mass * half) * (2.0 + jnp.tanh(mass))
                inflow = jnp.concatenate([jnp.zeros((1, SUB, LANE), jnp.float32), flux[:-1]], axis=0)
                mass = (mass + inflow) - flux
                fallen = fallen + flux[levels - 1]
            so[b, :, i] = mass
            dblk[pl.ds((b * tall + j) * SUB, SUB), :] = fallen

        with scope("settle"):
            for i in range(main):
                settle(i, lax.rem(me * main + i, tall))

            @pl.when(owned)
            def _():
                settle(main, extra_j)

        with scope("give_back"):
            for i in range(n_moves):
                give_back(b, i)
        for i in range(main):
            q2[b, me * each + i] = so[b, me, i]

        @pl.when(owned)
        def _():
            q2[b, me * each + main] = so[b, me, main]

    dts[...] = dblk[...].T

    def drop(i):
        return pltpu.make_async_remote_copy(
            dts.at[pl.ds(to(i) * lanes_each, lanes_each)], dr.at[me], d_sem.at[0], d_sem.at[1],
            device_id={"lev": to(i)}, device_id_type=MESH,
        )

    for i in range(n_moves):
        drop(i).start()
    dr[me] = dts[pl.ds(me * lanes_each, lanes_each), :]

    for b in range(bins):
        with scope("wait_back"):
            holder(b, b_sem, 1)
        zonal(2, b, q2)
        send_halo(2, b)

    for b in range(bins):
        wait_halo(2, b)
        meridional(b, rows_sent, keep_last)

    with scope("deposit"):
        all_drops = copy_to(0, dr.at[pl.ds(0, n_moves)], dr.at[pl.ds(0, n_moves)], d_sem.at[0], d_sem.at[1])
        all_drops.wait_recv()
        column = lax.broadcasted_iota(jnp.int32, (lanes_each, LANE), 1) // SUB
        low_rows = lax.rem(column, tall) < tall // 2
        for v in range(wide - 1):
            turn[pl.ds(v, lanes_each, stride=wide), :] = jnp.where(low_rows, dr[2 * v], dr[2 * v + 1])
        tail = jnp.zeros((lanes_each, LANE), jnp.float32)
        for g, (b, j) in enumerate(groups):
            t = (tall * b + 2 * (j % (tall // 2)) + (1 if j < tall // 2 else 0)) % levels
            tail = jnp.where(column == g, dr[t], tail)
        turn[pl.ds(wide - 1, lanes_each, stride=wide), :] = tail
        block = turn[:LANE, :].T
        for g, (b, j) in enumerate(groups):
            flat[bins + b, 0, pl.ds(j, SUB, stride=tall), :] = block[g * SUB : (g + 1) * SUB]
        for b in range(bins):
            deposit[b] = flat[bins + b, 0][:, :chunk]

    with scope("gather"):
        for v in range(wide):
            block = jnp.concatenate(
                [q3[b, v * tall + j] for b, j in groups] + [jnp.zeros((LANE - bins * rows, LANE), jnp.float32)], axis=0
            )
            turn[pl.ds(v, LANE, stride=wide), :] = block.T
        for v in range(wide):
            block = turn[v * LANE : (v + 1) * LANE, :].T
            for g, (b, j) in enumerate(groups):
                flat[b, v, pl.ds(j, SUB, stride=tall), :] = block[g * SUB : (g + 1) * SUB]
            for b in range(bins):
                out[b, :, v * LANE : (v + 1) * LANE] = flat[b, v]

    with scope("sent"):
        for side, there in ((0, has_north), (1, has_south)):
            @pl.when(there)
            def _():
                courants(side).wait_send()
                for kind, (source, target) in enumerate(((hs, hr), (hsf, hrf))):
                    pltpu.make_async_remote_copy(
                        source.at[side], target.at[side], hs_sem.at[kind, side], hr_sem.at[0, side, 0],
                        device_id=near(side), device_id_type=MESH,
                    ).wait_send()

        all_fall.wait_send()
        for b in range(bins):
            holder(b, w_sem, 0)
            settler(b, b_sem, 0)
        all_drops.wait_send()

def on_device(bands, levels, tracer, east, north, fall):
    bins, _, rows, width = tracer.shape
    tall, wide = rows // SUB, width // LANE
    chunk = width // levels
    main = tall * (wide - 1) // levels
    each = main + 1
    share = main * bins + (1 if bins * tall <= levels else bins)
    def lines(n):
        return -(-n * wide // SUB) * SUB

    f32 = jnp.float32
    field = VMEM((bins, wide * tall, SUB, LANE), f32)
    dealt = VMEM((bins, levels * each, SUB, LANE), f32)
    columns = VMEM((bins, levels, each, SUB, LANE), f32)
    out, deposit = pl.pallas_call(
        functools.partial(kernel, bands, levels),
        out_shape=(
            jax.ShapeDtypeStruct((bins, rows, width), f32),
            jax.ShapeDtypeStruct((bins, rows, chunk), f32),
        ),
        in_specs=[pl.BlockSpec(memory_space=pltpu.HBM)] * 4,
        out_specs=(pl.BlockSpec(memory_space=VMEM), pl.BlockSpec(memory_space=VMEM)),
        scratch_shapes=[
            VMEM((2 + 2 * bins, wide, rows, LANE), f32),
            VMEM((width, LANE), f32),
            dealt,
            field,
            dealt,
            field,
            VMEM((levels * share, SUB, LANE), f32),
            VMEM((3, tall, wide + 1, SUB, LANE), f32),
            VMEM((3, wide + 1, SUB, LANE), f32),
            VMEM((3, wide, tall + 7, SUB, LANE), f32),
            VMEM((bins, wide, SUB, LANE), f32),
            VMEM((bins, wide, SUB, LANE), f32),
            VMEM((2, 2, bins, lines(tall), LANE), f32),
            VMEM((2, 2, bins, lines(tall), LANE), f32),
            VMEM((2, bins, lines(3), LANE), f32),
            VMEM((2, bins, lines(3), LANE), f32),
            VMEM((2, lines(7), LANE), f32),
            VMEM((2, lines(7), LANE), f32),
            VMEM((wide, SUB, LANE), f32),
            VMEM((levels, share, SUB, LANE), f32),
            columns,
            columns,
            VMEM((LANE, LANE), f32),
            VMEM((LANE, LANE), f32),
            VMEM((levels, LANE // levels, LANE), f32),
            DMA((2 + 2 * bins,)),
            DMA((2, 2)),
            DMA((3, 2, bins)),
            DMA((2, 2)),
            DMA((2,)),
            DMA((2, bins)),
            DMA((2, bins)),
            DMA((2,)),
        ],
        compiler_params=pltpu.CompilerParams(collective_id=0, has_side_effects=True, vmem_limit_bytes=32 * 1024 * 1024),
        cost_estimate=pl.CostEstimate(flops=50000000, bytes_accessed=3000000, transcendentals=700000),
    )(
        *(
            pltpu.with_memory_space_constraint(array, pltpu.HBM)
            for array in (
                tracer.reshape(bins, rows, width),
                east.reshape(rows, width),
                north.reshape(rows, width),
                fall.reshape(bins, rows, width),
            )
        )
    )
    return out.reshape(tracer.shape), deposit


def solution(mesh):
    in_specs = (
        P(None, "lev", "lat", None),
        P("lev", "lat", None),
        P("lev", "lat", None),
        P(None, "lev", "lat", None),
    )
    out_specs = (P(None, "lev", "lat", None), P(None, "lat", "lev"))
    return jax.shard_map(
        functools.partial(on_device, mesh.shape["lat"], mesh.shape["lev"]),
        mesh=mesh, in_specs=in_specs, out_specs=out_specs, check_vma=False,
    )
```

```python
import functools

import jax
import jax.numpy as jnp
from jax import lax
from jax.experimental import pallas as pl
from jax.experimental.pallas import tpu as pltpu
from jax.sharding import PartitionSpec as P

HSUB = 4
SETTLE_SUBSTEPS = 6
SUB = 8
LANE = 128
MESH = pl.DeviceIdType.MESH
VMEM = pltpu.VMEM
DMA = pltpu.SemaphoreType.DMA
scope = jax.named_scope


def coefficients(k):
    s = jnp.abs(k)
    half = 0.5 * k * s
    a3 = 3.0 * half * (1.0 - (2.0 / 3.0) * s)
    return k - a3 - half, 2.0 * a3, half - a3


def swept(ext, c0, c1, c2):
    n = ext.shape[0] - 6
    b, c = ext[1 : n + 4], ext[2 : n + 5]
    face = (7.0 / 12.0) * (b + c) - (1.0 / 12.0) * (ext[: n + 3] + ext[3:])
    face = jnp.minimum(jnp.maximum(face, jnp.minimum(b, c)), jnp.maximum(b, c))
    up = c1 >= 0
    flux = (
        c0 * face[1 : n + 2]
        + c1 * jnp.where(up, ext[2 : n + 3], ext[3 : n + 4])
        + c2 * jnp.where(up, face[: n + 1], face[2:])
    )
    return ext[3 : n + 3] - (flux[1:] - flux[:-1])


def kernel(
    bands, levels,
    tracer, east, north, fall, out, deposit,
    flat, turn, q, z, q2, q3, fs, cz, czp, cm, p, zp, hs, hr, hsf, hrf, cs, cr, pe, rf, rw, so, dblk, dts, dr,
    in_sem, hs_sem, hr_sem, c_sem, f_sem, w_sem, b_sem, d_sem,
):
    bins, rows, width = tracer.shape
    tall = rows // SUB
    wide = width // LANE
    main = tall * (wide - 1) // levels
    each = main + 1
    spare = 1 if bins * tall <= levels else bins
    share = main * bins + spare
    across = levels // 4
    lanes_each = LANE // levels
    chunk = width // levels
    groups = [(b, j) for b in range(bins) for j in range(tall)]
    band = lax.axis_index("lat")
    me = lax.axis_index("lev")
    has_south, has_north = band > 0, band < bands - 1
    sub = lax.broadcasted_iota(jnp.int32, (SUB, LANE), 0)
    first, last = sub == 0, sub == SUB - 1

    half_at, x_at, core_at = me // (2 * across), lax.rem(me // 2, across), lax.rem(me, 2)
    moves = [
        (h, x, c)
        for h in (1, 0)
        for x in sorted(range(across), key=lambda x: -min(x, across - x))
        for c in range(2)
        if (h, x, c) != (0, 0, 0)
    ]
    n_moves = len(moves)
    same_half = [i for i, m in enumerate(moves) if m[0] == 0]
    other_half = [i for i, m in enumerate(moves) if m[0] == 1]

    def at(h, x, c):
        return (lax.rem(half_at + h, 2) * across + lax.rem(x_at + x, across)) * 2 + lax.rem(core_at + c, 2)

    def to(i):
        return at(*moves[i])

    def origin(i):
        h, x, c = moves[i]
        return at(h, across - x, c)

    barrier = pltpu.get_barrier_semaphore()
    for i in range(n_moves):
        pl.semaphore_signal(barrier, inc=1, device_id={"lev": to(i)}, device_id_type=MESH)

    @pl.when(has_south)
    def _():
        pl.semaphore_signal(barrier, inc=1, device_id={"lat": band - 1}, device_id_type=MESH)

    @pl.when(has_north)
    def _():
        pl.semaphore_signal(barrier, inc=1, device_id={"lat": band + 1}, device_id_type=MESH)

    def fetch(source, slot):
        return [
            pltpu.make_async_copy(
                source.at[:, pl.ds(v * LANE, LANE)], flat.at[slot, v], in_sem.at[slot]
            )
            for v in range(wide)
        ]

    fetched = [fetch(tracer.at[b], b) for b in range(bins)] + [fetch(east, bins), fetch(north, bins + 1)]
    fetched += [fetch(fall.at[b], bins + 2 + b) for b in range(bins)]
    for copies in fetched:
        for copy in copies:
            copy.start()

    for side, beyond in ((0, band == 0), (1, band == bands - 1)):
        @pl.when(beyond)
        def _():
            cr[side] = jnp.zeros(cr.shape[1:], jnp.float32)
            for b in range(bins):
                hrf[side, b] = jnp.zeros(hrf.shape[2:], jnp.float32)
                for e in range(2):
                    hr[side, e, b] = jnp.zeros(hr.shape[3:], jnp.float32)

    dblk[...] = jnp.zeros_like(dblk)

    def spread(slot, emit):
        for i in range(2):
            pltpu.make_async_copy(flat.at[slot + i], flat.at[slot + i], in_sem.at[slot + i]).wait()
        for v in range(wide):
            block = jnp.concatenate(
                [flat[slot + i, v, pl.ds(j, SUB, stride=tall), :] for i in range(2) for j in range(tall)]
                + [jnp.zeros((LANE - 2 * rows, LANE), jnp.float32)],
                axis=0,
            )
            turn[v * LANE : (v + 1) * LANE, :] = block.T
        for v in range(wide):
            block = turn[pl.ds(v, LANE, stride=wide), :].T
            for i in range(2):
                for j in range(tall):
                    start = (i * tall + j) * SUB
                    emit(i, j, v, block[start : start + SUB])

    def owner(b, j):
        half_tall = tall // 2
        return (tall * b + 2 * (j % half_tall) + (1 if j < half_tall else 0)) % levels

    def extra(b, t):
        u = lax.rem(t + levels * bins - tall * b, levels)
        return u < tall, u // 2 + (tall // 2) * (1 - lax.rem(u, 2))

    def place(b, v, j):
        tile = v * tall + j
        return (tile // main, tile % main) if v < wide - 1 else (owner(b, j), main)

    def index(b, v, j):
        t, i = place(b, v, j)
        return t * each + i

    def emit_tracer(b, j, v, tile):
        q[b, index(b, v, j)] = tile

    def emit_courant(i, j, v, tile):
        if i == 1 and j == tall - 1:
            tile = jnp.where(jnp.logical_and(last, band == bands - 1), 0.0, tile)
        sent, at_row = (3, 4) if i == 0 else (4, 0)
        if j >= tall - sent:
            cs[0, pl.ds((at_row + j - tall + sent) * wide + v, 1), :] = tile[SUB - 1 :, :]
        if j < 3:
            cs[1, pl.ds((at_row + j) * wide + v, 1), :] = tile[:1, :]
        for n, c in enumerate(coefficients(tile)):
            if i == 0:
                cz[n, j, v + 1] = c
            else:
                cm[n, v, j + 4] = c

    def emit_fall(b, j, v, tile):
        t, i = place(b, v, j)
        fs[t * share + (b * main + i if i < main else bins * main + b % spare)] = tile

    with scope("spread"):
        spread(0, emit_tracer)
        spread(bins, emit_courant)
        for n in range(3):
            for j in range(tall):
                cz[n, j, 0] = pltpu.roll(cz[n, j, wide], 1, 1)

    def near(side):
        return {"lat": band + 1 if side == 0 else band - 1}

    def courants(side):
        return pltpu.make_async_remote_copy(
            cs.at[side], cr.at[side], c_sem.at[0, side], c_sem.at[1, side], device_id=near(side), device_id_type=MESH
        )

    def halo(e, side, b):
        source, target = (hs.at[side, e, b], hr.at[side, e, b]) if e < 2 else (hsf.at[side, b], hrf.at[side, b])
        return pltpu.make_async_remote_copy(
            source, target, hs_sem.at[e // 2, side], hr_sem.at[e, side, b], device_id=near(side), device_id_type=MESH
        )

    def zonal_row(own, c0, c1, c2):
        ext = [pltpu.roll(t, 1, 1) for t in own[-3:]] + own + [pltpu.roll(t, LANE - 1, 1) for t in own[:3]]
        return swept(jnp.stack(ext), c0, c1, c2)

    def zonal(e, b, field):
        with scope("zonal"):
            for j in range(tall):
                new = zonal_row([field[b, index(b, v, j)] for v in range(wide)], cz[0, j], cz[1, j], cz[2, j])
                for v in range(wide):
                    z[b, v * tall + j] = new[v]
                    low, high = new[v][:1, :], new[v][SUB - 1 :, :]
                    if e in (0, 1):
                        hs[1, e, b, pl.ds(j * wide + v, 1), :] = low
                        hs[0, e, b, pl.ds(j * wide + v, 1), :] = high
                    elif e == 2 and j < 3:
                        hsf[1, b, pl.ds(j * wide + v, 1), :] = low
                    elif e == 2 and j >= tall - 3:
                        hsf[0, b, pl.ds((j - tall + 3) * wide + v, 1), :] = high
            if e is None:
                new = zonal_row([p[b, v] for v in range(wide)], czp[0], czp[1], czp[2])
                for v in range(wide):
                    zp[b, v] = new[v]

    def send_halo(e, b):
        @pl.when(has_north)
        def _():
            halo(e, 0, b).start()

        @pl.when(has_south)
        def _():
            halo(e, 1, b).start()

    def wait_halo(e, b):
        with scope("halo"):
            @pl.when(has_south)
            def _():
                halo(e, 0, b).wait_recv()

            @pl.when(has_north)
            def _():
                halo(e, 1, b).wait_recv()

    def extended(own, lows, highs):
        n = len(lows)
        below = [jnp.where(first, lows[i], pltpu.roll(own[tall - n + i], 1, 0)) for i in range(n)]
        above = [jnp.where(last, highs[i], pltpu.roll(own[i], SUB - 1, 0)) for i in range(n)]
        return jnp.stack(below + own + above)

    def meridional_wide(e, b):
        wait_halo(e, b)
        if e == 0 and b == bins - 1:
            send_fall(other_half[:3])
        with scope("meridional_wide"):
            for v in range(wide):
                own = [z[b, v * tall + j] for j in range(tall)]
                lows = [hr[0, e, b, pl.ds(i * wide + v, 1), :] for i in range(tall)]
                highs = [hr[1, e, b, pl.ds(i * wide + v, 1), :] for i in range(tall)]
                new = swept(extended(own, lows, highs), cm[0, v], cm[1, v], cm[2, v])
                for j in range(tall):
                    q[b, index(b, v, j)] = new[j + 3]
                for i in range(3):
                    p[b, v, i : i + 1, :] = new[i][:1, :]
                    p[b, v, i + 3 : i + 4, :] = new[tall + 3 + i][SUB - 1 :, :]

    def meridional(b, rows_of, keep):
        with scope("meridional"):
            for v in range(wide):
                own = [z[b, v * tall + j] for j in range(tall)]
                lows, highs = rows_of(b, v)
                c0, c1, c2 = [cm[n, v, 3 : tall + 4] for n in range(3)]
                new = swept(extended(own, lows, highs), c0, c1, c2)
                for j in range(tall):
                    keep(b, v, j, new[j])

    def rows_kept(b, v):
        return [zp[b, v, i : i + 1, :] for i in range(3)], [zp[b, v, i + 3 : i + 4, :] for i in range(3)]

    def rows_sent(b, v):
        return [[hrf[side, b, pl.ds(i * wide + v, 1), :] for i in range(3)] for side in range(2)]

    def keep_mass(b, v, j, tile):
        q[b, index(b, v, j)] = tile

    def keep_last(b, v, j, tile):
        q3[b, v * tall + j] = tile

    def copy_to(i, source, target, send, recv):
        return pltpu.make_async_remote_copy(
            source, target, send, recv, device_id={"lev": to(i)}, device_id_type=MESH
        )

    def either(condition, yes, no):
        @pl.when(condition)
        def _():
            yes()

        @pl.when(jnp.logical_not(condition))
        def _():
            no()

    def deal_fall(i):
        return copy_to(i, fs.at[pl.ds(to(i) * share, share)], rf.at[me], f_sem.at[0], f_sem.at[1])

    def deal_mass(b, i):
        t = to(i)
        send, recv = w_sem.at[0, b], w_sem.at[1, b]
        either(
            extra(b, t)[0],
            copy_to(i, q.at[b, pl.ds(t * each, each)], rw.at[b, me], send, recv).start,
            copy_to(i, q.at[b, pl.ds(t * each, main)], rw.at[b, me, pl.ds(0, main)], send, recv).start,
        )

    def give_back(b, i):
        t = to(i)
        send, recv = b_sem.at[0, b], b_sem.at[1, b]
        either(
            extra(b, me)[0],
            copy_to(i, so.at[b, t], q2.at[b, pl.ds(me * each, each)], send, recv).start,
            copy_to(i, so.at[b, t, pl.ds(0, main)], q2.at[b, pl.ds(me * each, main)], send, recv).start,
        )

    def settler(b, sems, side):
        full, part = rw.at[b, pl.ds(0, n_moves)], rw.at[b, pl.ds(0, n_moves), pl.ds(0, main)]
        name = "wait_recv" if side else "wait_send"
        either(
            extra(b, me)[0],
            getattr(copy_to(0, full, full, sems.at[0, b], sems.at[1, b]), name),
            getattr(copy_to(0, part, part, sems.at[0, b], sems.at[1, b]), name),
        )

    def holder(b, sems, side):
        count = n_moves * main + tall
        few, many = q.at[b, pl.ds(0, count - 1)], q.at[b, pl.ds(0, count)]
        name = "wait_recv" if side else "wait_send"
        either(
            extra(b, me)[0],
            getattr(copy_to(0, few, few, sems.at[0, b], sems.at[1, b]), name),
            getattr(copy_to(0, many, many, sems.at[0, b], sems.at[1, b]), name),
        )

    all_fall = copy_to(0, rf.at[pl.ds(0, n_moves)], rf.at[pl.ds(0, n_moves)], f_sem.at[0], f_sem.at[1])

    def send_fall(some):
        for i in some:
            deal_fall(i).start()

    for b in range(bins):
        p[b] = jnp.zeros(p.shape[1:], jnp.float32)
    pe[...] = jnp.zeros_like(pe)
    for b in range(bins):
        zonal(0, b, q)
    with scope("spread_fall"):
        spread(bins + 2, emit_fall)
    with scope("barrier"):
        pl.semaphore_wait(barrier, n_moves + has_south.astype(jnp.int32) + has_north.astype(jnp.int32))

    @pl.when(has_north)
    def _():
        courants(0).start()

    @pl.when(has_south)
    def _():
        courants(1).start()

    for b in range(bins):
        send_halo(0, b)
    for i in range(share):
        rf[me, i] = fs[me * share + i]

    with scope("courants"):
        @pl.when(has_south)
        def _():
            courants(0).wait_recv()

        @pl.when(has_north)
        def _():
            courants(1).wait_recv()

    with scope("edge_coefficients"):
        for v in range(wide):
            for i in range(4):
                low = coefficients(cr[0, pl.ds(i * wide + v, 1), :])
                for n in range(3):
                    cm[n, v, i] = jnp.where(first, low[n], pltpu.roll(cm[n, v, i + tall], 1, 0))
            for i in range(3):
                high = coefficients(cr[1, pl.ds(i * wide + v, 1), :])
                for n in range(3):
                    cm[n, v, tall + 4 + i] = jnp.where(last, high[n], pltpu.roll(cm[n, v, i + 4], SUB - 1, 0))
                pe[v, i : i + 1, :] = cr[0, pl.ds((4 + i) * wide + v, 1), :]
                pe[v, i + 3 : i + 4, :] = cr[1, pl.ds((4 + i) * wide + v, 1), :]
        for v in range(wide):
            for n, c in enumerate(coefficients(pe[v])):
                czp[n, v + 1] = c
        for n in range(3):
            czp[n, 0] = pltpu.roll(czp[n, wide], 1, 1)

    for e in range(HSUB // 2):
        if e:
            for b in range(bins):
                zonal(e, b, q)
                send_halo(e, b)
            send_fall(same_half + other_half[3:])
        for b in range(bins):
            meridional_wide(e, b)
            zonal(None, b, q)
            meridional(b, rows_kept, keep_mass)
            if e == HSUB // 2 - 1:
                for i in range(n_moves):
                    deal_mass(b, i)

    for b in range(bins):
        owned, extra_j = extra(b, me)
        for i in range(main):
            rw[b, me, i] = q[b, me * each + i]

        @pl.when(owned)
        def _():
            rw[b, me, main] = q[b, me * each + main]

        if b == 0:
            with scope("wait_fall"):
                all_fall.wait_recv()
        with scope("wait_mass"):
            settler(b, w_sem, 1)

        def settle(i, j):
            mass = rw[b, :, i]
            half = 0.5 * rf[:, b * main + i if i < main else bins * main + b % spare]
            fallen = jnp.zeros((SUB, LANE), jnp.float32)
            for _ in range(SETTLE_SUBSTEPS):
                flux = (mass * half) * (2.0 + jnp.tanh(mass))
                inflow = jnp.concatenate([jnp.zeros((1, SUB, LANE), jnp.float32), flux[:-1]], axis=0)
                mass = (mass + inflow) - flux
                fallen = fallen + flux[levels - 1]
            so[b, :, i] = mass
            dblk[pl.ds((b * tall + j) * SUB, SUB), :] = fallen

        with scope("settle"):
            for i in range(main):
                settle(i, lax.rem(me * main + i, tall))

            @pl.when(owned)
            def _():
                settle(main, extra_j)

        with scope("give_back"):
            for i in range(n_moves):
                give_back(b, i)
        for i in range(main):
            q2[b, me * each + i] = so[b, me, i]

        @pl.when(owned)
        def _():
            q2[b, me * each + main] = so[b, me, main]

    dts[...] = dblk[...].T

    def drop(i):
        return pltpu.make_async_remote_copy(
            dts.at[pl.ds(to(i) * lanes_each, lanes_each)], dr.at[me], d_sem.at[0], d_sem.at[1],
            device_id={"lev": to(i)}, device_id_type=MESH,
        )

    for i in range(n_moves):
        drop(i).start()
    dr[me] = dts[pl.ds(me * lanes_each, lanes_each), :]

    for b in range(bins):
        with scope("wait_back"):
            holder(b, b_sem, 1)
        zonal(2, b, q2)
        send_halo(2, b)

    for b in range(bins):
        wait_halo(2, b)
        meridional(b, rows_sent, keep_last)

    with scope("deposit"):
        all_drops = copy_to(0, dr.at[pl.ds(0, n_moves)], dr.at[pl.ds(0, n_moves)], d_sem.at[0], d_sem.at[1])
        all_drops.wait_recv()
        column = lax.broadcasted_iota(jnp.int32, (lanes_each, LANE), 1) // SUB
        low_rows = lax.rem(column, tall) < tall // 2
        for v in range(wide - 1):
            turn[pl.ds(v, lanes_each, stride=wide), :] = jnp.where(low_rows, dr[2 * v], dr[2 * v + 1])
        tail = jnp.zeros((lanes_each, LANE), jnp.float32)
        for g, (b, j) in enumerate(groups):
            t = (tall * b + 2 * (j % (tall // 2)) + (1 if j < tall // 2 else 0)) % levels
            tail = jnp.where(column == g, dr[t], tail)
        turn[pl.ds(wide - 1, lanes_each, stride=wide), :] = tail
        block = turn[:LANE, :].T
        for g, (b, j) in enumerate(groups):
            flat[bins + b, 0, pl.ds(j, SUB, stride=tall), :] = block[g * SUB : (g + 1) * SUB]
        for b in range(bins):
            deposit[b] = flat[bins + b, 0][:, :chunk]

    with scope("gather"):
        for v in range(wide):
            block = jnp.concatenate(
                [q3[b, v * tall + j] for b, j in groups] + [jnp.zeros((LANE - bins * rows, LANE), jnp.float32)], axis=0
            )
            turn[pl.ds(v, LANE, stride=wide), :] = block.T
        for v in range(wide):
            block = turn[v * LANE : (v + 1) * LANE, :].T
            for g, (b, j) in enumerate(groups):
                flat[b, v, pl.ds(j, SUB, stride=tall), :] = block[g * SUB : (g + 1) * SUB]
            for b in range(bins):
                out[b, :, v * LANE : (v + 1) * LANE] = flat[b, v]

    with scope("sent"):
        for side, there in ((0, has_north), (1, has_south)):
            @pl.when(there)
            def _():
                courants(side).wait_send()
                for kind, (source, target) in enumerate(((hs, hr), (hsf, hrf))):
                    pltpu.make_async_remote_copy(
                        source.at[side], target.at[side], hs_sem.at[kind, side], hr_sem.at[0, side, 0],
                        device_id=near(side), device_id_type=MESH,
                    ).wait_send()

        all_fall.wait_send()
        for b in range(bins):
            holder(b, w_sem, 0)
            settler(b, b_sem, 0)
        all_drops.wait_send()

def on_device(bands, levels, tracer, east, north, fall):
    bins, _, rows, width = tracer.shape
    tall, wide = rows // SUB, width // LANE
    chunk = width // levels
    main = tall * (wide - 1) // levels
    each = main + 1
    share = main * bins + (1 if bins * tall <= levels else bins)
    def lines(n):
        return -(-n * wide // SUB) * SUB

    f32 = jnp.float32
    field = VMEM((bins, wide * tall, SUB, LANE), f32)
    dealt = VMEM((bins, levels * each, SUB, LANE), f32)
    columns = VMEM((bins, levels, each, SUB, LANE), f32)
    out, deposit = pl.pallas_call(
        functools.partial(kernel, bands, levels),
        out_shape=(
            jax.ShapeDtypeStruct((bins, rows, width), f32),
            jax.ShapeDtypeStruct((bins, rows, chunk), f32),
        ),
        in_specs=[pl.BlockSpec(memory_space=pltpu.HBM)] * 4,
        out_specs=(pl.BlockSpec(memory_space=VMEM), pl.BlockSpec(memory_space=VMEM)),
        scratch_shapes=[
            VMEM((2 + 2 * bins, wide, rows, LANE), f32),
            VMEM((width, LANE), f32),
            dealt,
            field,
            dealt,
            field,
            VMEM((levels * share, SUB, LANE), f32),
            VMEM((3, tall, wide + 1, SUB, LANE), f32),
            VMEM((3, wide + 1, SUB, LANE), f32),
            VMEM((3, wide, tall + 7, SUB, LANE), f32),
            VMEM((bins, wide, SUB, LANE), f32),
            VMEM((bins, wide, SUB, LANE), f32),
            VMEM((2, 2, bins, lines(tall), LANE), f32),
            VMEM((2, 2, bins, lines(tall), LANE), f32),
            VMEM((2, bins, lines(3), LANE), f32),
            VMEM((2, bins, lines(3), LANE), f32),
            VMEM((2, lines(7), LANE), f32),
            VMEM((2, lines(7), LANE), f32),
            VMEM((wide, SUB, LANE), f32),
            VMEM((levels, share, SUB, LANE), f32),
            columns,
            columns,
            VMEM((LANE, LANE), f32),
            VMEM((LANE, LANE), f32),
            VMEM((levels, LANE // levels, LANE), f32),
            DMA((2 + 2 * bins,)),
            DMA((2, 2)),
            DMA((3, 2, bins)),
            DMA((2, 2)),
            DMA((2,)),
            DMA((2, bins)),
            DMA((2, bins)),
            DMA((2,)),
        ],
        compiler_params=pltpu.CompilerParams(collective_id=0, has_side_effects=True, vmem_limit_bytes=32 * 1024 * 1024),
        cost_estimate=pl.CostEstimate(flops=50000000, bytes_accessed=3000000, transcendentals=700000),
    )(
        *(
            pltpu.with_memory_space_constraint(array, pltpu.HBM)
            for array in (
                tracer.reshape(bins, rows, width),
                east.reshape(rows, width),
                north.reshape(rows, width),
                fall.reshape(bins, rows, width),
            )
        )
    )
    return out.reshape(tracer.shape), deposit


def solution(mesh):
    in_specs = (
        P(None, "lev", "lat", None),
        P("lev", "lat", None),
        P("lev", "lat", None),
        P(None, "lev", "lat", None),
    )
    out_specs = (P(None, "lev", "lat", None), P(None, "lat", "lev"))
    return jax.shard_map(
        functools.partial(on_device, mesh.shape["lat"], mesh.shape["lev"]),
        mesh=mesh, in_specs=in_specs, out_specs=out_specs, check_vma=False,
    )
```
